32 devices in a mesh: shots: 2 (over x), mx: 16 (over z, y, core).
Axes of the slice: x: 2, y: 2, z: 4, core: 2. Of those that a mesh axis runs over, the one named last changes fastest.
Arguments:
- initial: float32 [18, 125, 2048], P('shots', None, 'mx'), parts along dimension 0, may hold values from -6 to 6
- derivative: float32 [3, 125, 125], replicated, may hold values from -0.5 to 0.5
- coupling: float32 [3, 9, 9], replicated, may hold values from -2 to 2
- face_lift: float32 [2, 125, 125], replicated, may hold values from -0.5 to 0.5
- metric: float32 [3, 2048], P(None, 'mx'), may hold values from 0.3 to 3
- rec_element: int32 [4096], P('mx'), may hold values from 0 to 127
- rec_weight: float32 [125, 4096], P(None, 'mx'), may hold values from -0.5 to 0.5
- live_counts: int32 [16], replicated, may hold values from 1 to 256, 2048 in all
- shot_order: int32 [4096], replicated, may hold values from 0 to 4095, as said below
- observed: float32 [8192, 48], P(('shots', 'mx')), parts along dimension 0, may hold values from -6 to 6
Outputs:
- residual: float32 [8192, 48], P(('shots', 'mx')), parts along dimension 0
- misfit: float32 [8192], P(('shots', 'mx')), parts along dimension 0
- adjoint: float32 [8192, 48], P(('shots', 'mx')), parts along dimension 0
The draws below stay inside these ranges and needn't reach their ends.
There are 2 independent parts, one for each index of `shots`. The reference program is written for one: setup_inputs(seed, part) draws one part's arguments, and reference() takes and returns one part's arrays. A program takes and returns all parts, laid end to end along the dimension named above; an argument that names none is the same for every part. Nothing has to cross between parts.
Inputs may be any that keep to these rules, and one draw needn't show every extreme that they name: `rec_element`: local element index of the slot within its block of 128 elements. The live receivers of block b are its first live_counts[b] slots. `shot_order`: a permutation of the slots; of the 256 positions of each block of shot-receiver order, exactly 16 come from the slots of each block.
All inputs are finite; a program needn't handle non-finite values.
Results may differ from the reference program's by a relative error of at most 0.00018.
Values sent between devices are 32-bit elements; how exact they have to be, the bound alone decides.
A program may use at most 64 MiB of HBM per device.

```python
import math
import jax
import jax.numpy as jnp
import numpy as np
from jax import lax

FIELDS = 9
NODE = 125
STEPS = 12
E_DEV = 128
R_DEV = 256
TW = 48
BLOCKS = 16
PAIR = 16
ELEMS = 2048
R_TOTAL = 4096


def draw_shot_order(key, part):
    key_a, key_b = jax.random.split(key)
    slot_perm = jax.vmap(lambda sub: jax.random.permutation(sub, R_DEV))(jax.random.split(key_a, BLOCKS))
    grouped = slot_perm.reshape(BLOCKS, BLOCKS, PAIR)
    source_ids = jnp.arange(BLOCKS, dtype=jnp.int32)[:, None, None] * R_DEV + grouped.astype(jnp.int32)
    per_dest = source_ids.transpose(1, 0, 2).reshape(BLOCKS, R_DEV)
    dest_order = jax.vmap(lambda sub: jax.random.permutation(sub, R_DEV))(jax.random.split(key_b, BLOCKS))
    placed = jnp.take_along_axis(per_dest, dest_order.astype(jnp.int32), axis=1)
    return placed.reshape(-1).astype(jnp.int32)


def with_ends(drawn, rng, least, largest):
    longest = drawn.shape.index(max(drawn.shape))
    spots = []
    for shift in (0, 1):
        where = [jax.random.randint(jax.random.fold_in(rng, axis), (), 0, length) for axis, length in enumerate(drawn.shape)]
        where[longest] = (where[longest] + shift) % drawn.shape[longest]
        spots.append(tuple(where))
    return drawn.at[spots[0]].set(least).at[spots[1]].set(largest)


def level_of(key, extent, pieces, low, high):
    loudness = 1.0
    for position, shards_of in pieces:
        heights = jax.random.uniform(jax.random.fold_in(jax.random.fold_in(key, 6), position), (shards_of,), jnp.float32, low / len(pieces), high / len(pieces))
        loudness = loudness * jnp.repeat(jnp.exp(heights), extent[position] // shards_of).reshape((-1,) + (1,) * (len(extent) - 1 - position))
    return loudness


def split_up(count, total, most, slope):
    loads = [(1 << 20) // math.isqrt(standing ** slope) + 1 for standing in range(2, count + 1)]
    spare, counts = total - most - (count - 1), [1] * (count - 1)
    while spare > 0:
        free = [i for i in range(count - 1) if counts[i] < most]
        pool, left = sum([loads[i] for i in free]), spare
        for i in free:
            extra = min(most - counts[i], max(1, left * loads[i] // pool), spare)
            counts[i] = counts[i] + extra
            spare = spare - extra
    return np.array([most] + counts)


def ragged_sizes(stream_key, number_of, total, limit, lean):
    if number_of == 2:
        one = jax.random.randint(stream_key, (), max(1, total - limit), min(limit, total - 1) + 1)
        return jnp.stack([one, total - one])
    tallies = jnp.asarray(split_up(number_of, total, limit, lean), jnp.int32)
    pairs = (number_of - 1) // 2
    donor, receiver = tallies[1:1 + 2 * pairs:2], tallies[2:2 + 2 * pairs:2]
    margin = jnp.minimum(donor - 1, limit - receiver)
    passed = jax.random.randint(jax.random.fold_in(stream_key, 1), (pairs,), 0, 1 << 20) % (margin + 1)
    tallies = tallies.at[1:1 + 2 * pairs:2].set(donor - passed).at[2:2 + 2 * pairs:2].set(receiver + passed)
    return tallies[jax.random.permutation(jax.random.fold_in(stream_key, 2), number_of)]


def normal_values(own_key, extent, spread, most, pieces=(), kind=jnp.bfloat16):
    result = spread * jax.random.normal(own_key, extent, jnp.float32)
    if pieces:
        result = result * level_of(own_key, extent, pieces, -0.22, 0.18)
    return jnp.clip(result, -most, most).astype(kind)


def setup_inputs(seed: int = 0, part: int = 0) -> dict:
    key_list = jax.random.split(jax.random.key(seed), 11)
    part_splits = jax.random.split(jax.random.fold_in(key_list[10], part), 11)
    initial = normal_values(part_splits[0], (FIELDS, NODE, ELEMS), 1.0, 6.0, ((2, 16),), jnp.float32)
    derivative = normal_values(key_list[1], (3, NODE, NODE), NODE ** -0.5, 0.5, (), jnp.float32)
    coupling = normal_values(key_list[2], (3, FIELDS, FIELDS), FIELDS ** -0.5, 2.0, (), jnp.float32)
    face_lift = normal_values(key_list[3], (2, NODE, NODE), NODE ** -0.5, 0.5, (), jnp.float32)
    metric = jnp.clip(jnp.exp(math.log(3.0) - 2.3025851 * jax.random.uniform(key_list[4], (3, ELEMS), jnp.float32) ** level_of(key_list[4], (3, ELEMS), ((1, 16),), -0.2, 0.2)), 0.3, 3.0)
    rec_element = with_ends(jax.random.randint(key_list[5], (R_TOTAL,), 0, E_DEV), jax.random.fold_in(key_list[5], 1), 0, E_DEV - 1).astype(jnp.int32)
    rec_weight = normal_values(key_list[6], (NODE, R_TOTAL), NODE ** -0.5, 0.5, ((1, 16),), jnp.float32)
    live_counts = ragged_sizes(key_list[7], BLOCKS, BLOCKS * R_DEV // 2, R_DEV, 2).astype(jnp.int32)
    shot_order = draw_shot_order(jax.random.fold_in(key_list[10], 71), part)
    observed = normal_values(part_splits[9], (R_TOTAL, TW), 1.0, 6.0, ((0, 16),), jnp.float32)
    return dict(initial=initial, derivative=derivative, coupling=coupling, face_lift=face_lift, metric=metric, rec_element=rec_element, rec_weight=rec_weight, live_counts=live_counts, shot_order=shot_order, observed=observed)


HIGH = lax.Precision.HIGHEST


def advance(extended, metric_cols, derivative, coupling, face_lift, time_step):
    middle = extended[:, :, 1:-1]
    summed = jnp.einsum('pq,fqe->fpe', face_lift[0], extended[:, :, :-2] - middle, precision=HIGH)
    summed = summed + jnp.einsum('pq,fqe->fpe', face_lift[1], extended[:, :, 2:] - middle, precision=HIGH)
    for k in range(3):
        gradient = jnp.einsum('pq,fqe->fpe', derivative[k], middle, precision=HIGH)
        summed = summed + jnp.einsum('gf,fpe->gpe', coupling[k], gradient, precision=HIGH) * metric_cols[k][None, None, :]
    return middle + time_step * summed


def sample(wavefield, elements, rec_weight, live_slot):
    components = jnp.stack([wavefield[0], wavefield[1], wavefield[2], (wavefield[3] + wavefield[4] + wavefield[5]) / 3.0])
    columns = jnp.take(components, elements, axis=2)
    return jnp.sum(columns * rec_weight[None], axis=1) * live_slot[None]


def reference(initial, derivative, coupling, face_lift, metric, rec_element, rec_weight, live_counts, shot_order, observed):
    time_step = 0.5 / STEPS
    slot_ids = jnp.arange(R_TOTAL, dtype=jnp.int32)
    block_of = slot_ids // R_DEV
    global_elem = (block_of * E_DEV + rec_element).astype(jnp.int32)
    live_slot = ((slot_ids % R_DEV) < live_counts[block_of]).astype(jnp.float32)

    def one_step(t, carry):
        wavefield, trace_buffer = carry
        extended = jnp.pad(wavefield, ((0, 0), (0, 0), (1, 1)))
        wavefield = advance(extended, metric, derivative, coupling, face_lift, time_step)
        sampled = sample(wavefield, global_elem, rec_weight, live_slot)
        trace_buffer = lax.dynamic_update_slice(trace_buffer, sampled[:, None, :], (0, t, 0))
        return wavefield, trace_buffer

    trace_buffer = jnp.zeros((4, STEPS, R_TOTAL), jnp.float32)
    final_field, trace_buffer = lax.fori_loop(0, STEPS, one_step, (initial, trace_buffer))
    synthetic = trace_buffer.transpose(2, 0, 1).reshape(R_TOTAL, 4 * STEPS)
    ordered = synthetic[shot_order]
    live_out = live_slot[shot_order]
    residual = live_out[:, None] * (ordered - observed)
    misfit = 0.5 * jnp.sum(residual * residual, axis=1)
    flipped = residual.reshape(R_TOTAL, 4, STEPS)[:, :, ::-1].reshape(R_TOTAL, 4 * STEPS)
    adjoint = jnp.zeros_like(flipped).at[shot_order].set(flipped)
    return residual, misfit, adjoint
```

```python
import functools
import jax
import jax.numpy as jnp
from jax import lax
from jax.experimental import pallas as pl
from jax.experimental.pallas import tpu as pltpu
from jax.sharding import PartitionSpec as P

STEPS = 12
COMPS = 4
HALO = 16
GUARD = 8
TILE = 16
SUB = 8
AHEAD = 3
WIDE = 4


def split(x):
    hi = x.astype(jnp.bfloat16)
    return hi, (x - hi.astype(jnp.float32)).astype(jnp.bfloat16)


def zeros(*shape):
    return jnp.zeros(shape, jnp.float32)


def ones_where(cond):
    return jnp.where(cond, 1.0, 0.0).astype(jnp.bfloat16)


def dot(a, b):
    return jnp.dot(a, b, preferred_element_type=jnp.float32)


def permute(onehot, x):
    hi = x.astype(jnp.bfloat16)
    rest = x - hi.astype(jnp.float32)
    mid = rest.astype(jnp.bfloat16)
    low = (rest - mid.astype(jnp.float32)).astype(jnp.bfloat16)
    return dot(onehot, hi) + (dot(onehot, mid) + dot(onehot, low))


def greet(peers, me):
    barrier = pltpu.get_barrier_semaphore()

    def one(off, _):
        pl.semaphore_signal(barrier, inc=1, device_id={"mx": lax.rem(me + off, peers)}, device_id_type=pl.DeviceIdType.MESH)
        return 0

    lax.fori_loop(1, peers, one, 0)
    return barrier


def start_kernel(peers, initial, metric, derivative, face_lift, weight_in, order, counts,
                 state, wb, ws, to_send, from_send, to_place, from_place, live,
                 pad, padw, send_sem, recv_sem):
    fields, nodes, count = initial.shape
    lanes = pad.shape[0]
    slots = order.shape[1]
    pair = slots // peers
    me = lax.axis_index("mx")
    right, left = lax.rem(me + 1, peers), lax.rem(me + peers - 1, peers)
    barrier = pltpu.get_barrier_semaphore()
    for side in (left, right):
        pl.semaphore_signal(barrier, inc=1, device_id={"mx": side}, device_id_type=pl.DeviceIdType.MESH)
    pad[...] = zeros(lanes, lanes)
    for f in range(fields):
        pad[0:nodes, :] = initial[f]
        state[f, HALO:HALO + count] = pad[...].T
    kinds = metric.shape[0]
    for k in range(kinds):
        state[fields + k, HALO:HALO + count] = jnp.broadcast_to(metric[k:k + 1, :], (lanes, count)).T
    pl.semaphore_wait(barrier, 2)
    moved = fields + kinds
    copies = []
    for i, (side, at, to) in enumerate(((right, count, 0), (left, HALO, HALO + count))):
        copies.append(pltpu.make_async_remote_copy(
            src_ref=state.at[0:moved, at:at + HALO], dst_ref=state.at[0:moved, to:to + HALO],
            send_sem=send_sem.at[i], recv_sem=recv_sem.at[i],
            device_id={"mx": side}, device_id_type=pl.DeviceIdType.MESH))
        copies[-1].start()
    pad[...] = zeros(lanes, lanes)
    turns = derivative.shape[0]

    def weigh(k, matrix):
        pad[0:nodes, 0:nodes] = matrix
        hi, lo = split(pad[...].T * (0.5 / STEPS))
        at = slice(k * lanes, (k + 1) * lanes)
        wb[0:lanes, at] = hi
        wb[lanes:2 * lanes, at] = hi
        wb[2 * lanes:, at] = lo

    for k in range(turns):
        weigh(k, derivative[k])
    weigh(turns, face_lift[0])
    weigh(turns + 1, face_lift[1])
    weigh(turns + 2, -(face_lift[0] + face_lift[1]))
    padw[...] = zeros(lanes, slots)
    padw[0:nodes, :] = weight_in[...]
    hi, lo = split(padw[...])
    ws[0:lanes] = hi
    ws[lanes:2 * lanes] = hi
    ws[2 * lanes:] = lo
    rows = lax.broadcasted_iota(jnp.int32, (count + 2 * HALO, lanes), 0) + (me * count - HALO)
    state[moved] = jnp.where((rows >= 0) & (rows < count * peers), 1.0, 0.0)

    up = lax.broadcasted_iota(jnp.int32, (slots, slots), 0)
    across = lax.broadcasted_iota(jnp.int32, (slots, slots), 1)
    tri = ones_where(up <= across)
    blocks = order[...]
    source, slot = lax.div(blocks, slots), lax.rem(blocks, slots)
    mine = source == me
    rank = dot(ones_where(mine), tri) - 1.0
    rank = jnp.where(mine, rank, -1.0)
    tall = lax.broadcasted_iota(jnp.int32, (slots, peers), 0)
    wide = lax.broadcasted_iota(jnp.int32, (slots, peers), 1)
    repeat = ones_where(lax.div(tall, pair) == wide)
    rank_all = dot(repeat, rank.astype(jnp.bfloat16))
    slot_all = dot(repeat, slot.astype(jnp.float32).astype(jnp.bfloat16))
    hit = rank_all == lax.rem(up, pair).astype(jnp.float32)
    send_slot = jnp.sum(jnp.where(hit, slot_all, 0.0), axis=1, keepdims=True)
    sends = jnp.where(send_slot == across.astype(jnp.float32), 1.0, 0.0)
    to_send[...] = sends.astype(jnp.bfloat16)
    from_send[...] = sends.T.astype(jnp.bfloat16)
    own = order[pl.ds(me, 1), :]
    own_source = lax.div(own, slots)
    peer_ids = lax.broadcasted_iota(jnp.int32, (peers, slots), 0)
    from_peer = peer_ids == own_source
    seen = dot(ones_where(from_peer), tri) - 1.0
    own_rank = jnp.sum(jnp.where(from_peer, seen, 0.0), axis=0, keepdims=True)
    place = own_source.astype(jnp.float32) * float(pair) + own_rank
    places = jnp.where(up.astype(jnp.float32) == place, 1.0, 0.0)
    to_place[...] = places.astype(jnp.bfloat16)
    from_place[...] = places.T.astype(jnp.bfloat16)
    here = lax.broadcasted_iota(jnp.int32, (1, peers), 1) == me
    limit = jnp.sum(jnp.where(here, counts[...].astype(jnp.float32), 0.0), axis=1, keepdims=True)
    live[...] = jnp.where(lax.broadcasted_iota(jnp.int32, (1, slots), 1).astype(jnp.float32) < limit, 1.0, 0.0)
    for copy in copies:
        copy.wait()


def end_kernel(peers, traces, observed, to_send, from_send, to_place, from_place,
               residual, misfit, adjoint, sent, got, send_sem, recv_sem):
    width, slots = observed.shape
    lanes = sent.shape[-1]
    wide = traces.shape[0]
    pair = slots // peers
    me = lax.axis_index("mx")
    barrier = greet(peers, me)
    synth = traces[...].T
    packed = permute(to_send[...], synth)
    obs = permute(to_place[...], observed[...].T)
    row = jnp.concatenate([packed, obs, zeros(slots, lanes - wide - width)], axis=1)
    sent[...] = row.reshape(peers, pair, lanes)
    pl.semaphore_wait(barrier, peers - 1)

    def copy_to(off):
        dest = lax.rem(me + off, peers)
        return pltpu.make_async_remote_copy(
            src_ref=sent.at[dest], dst_ref=got.at[me], send_sem=send_sem.at[dest], recv_sem=recv_sem.at[me],
            device_id={"mx": dest}, device_id_type=pl.DeviceIdType.MESH)

    def copy_from(off):
        src = lax.rem(me - off + peers, peers)
        return pltpu.make_async_remote_copy(
            src_ref=sent.at[src], dst_ref=got.at[src], send_sem=send_sem.at[src], recv_sem=recv_sem.at[src],
            device_id={"mx": src}, device_id_type=pl.DeviceIdType.MESH)

    def begin(off, _):
        copy_to(off).start()
        return 0

    def finish(off, _):
        copy_from(off).wait_recv()
        return 0

    def drain(off, _):
        copy_to(off).wait_send()
        return 0

    lax.fori_loop(1, peers, begin, 0)
    got[pl.ds(me, 1)] = sent[pl.ds(me, 1)]
    lax.fori_loop(1, peers, finish, 0)
    arrived = got[...].reshape(slots, lanes)
    placed = permute(from_place[...], arrived[:, :wide]).T
    res = placed[width:width + 1] * (placed[:width] - observed[...])
    residual[...] = res
    misfit[...] = 0.5 * jnp.sum(res * res, axis=0, keepdims=True)
    slot_obs = permute(from_send[...], arrived[:, wide:wide + width]).T
    plain = traces[width:width + 1, :] * (traces[0:width, :] - slot_obs)
    a = lax.broadcasted_iota(jnp.int32, (width, width), 0)
    b = lax.broadcasted_iota(jnp.int32, (width, width), 1)
    back = ones_where((lax.div(a, STEPS) == lax.div(b, STEPS)) & (lax.rem(a, STEPS) + lax.rem(b, STEPS) == STEPS - 1))
    adjoint[...] = permute(back, plain)
    lax.fori_loop(1, peers, drain, 0)


def wave_kernel(state, wb, ws, elem, live, cpl, out, u, x, xp, turned, faces, pick, rows_out, mixer):
    fields, total, lanes = u.shape
    span = state.shape[1]
    count = span - 2 * HALO
    kinds = turned.shape[0] - 1
    margin = (total - span) // 2
    own = margin + HALO
    slots = ws.shape[1]
    groups = total // TILE

    def stored(f, r, n):
        return state[f, r - margin:r - margin + n]

    def put(grp, f, new):
        hi, lo = split(new)
        x[grp, f * TILE:(f + 1) * TILE, 0:lanes] = hi
        x[grp, f * TILE:(f + 1) * TILE, lanes:] = lo

    for f in range(fields):
        u[f, 0:margin] = zeros(margin, lanes)
        u[f, total - margin:] = zeros(margin, lanes)
        u[f, margin:total - margin] = state[f] * state[fields + kinds]
        for k in range(2):
            faces[k, f, 0:GUARD] = zeros(GUARD, lanes)
            faces[k, f, GUARD + total:] = zeros(GUARD, lanes)
        for grp in range(groups):
            put(grp, f, u[f, grp * TILE:(grp + 1) * TILE])

    for i in range(mixer.shape[0]):
        mixer[i] = jnp.full((SUB, lanes), cpl[i], jnp.float32)
    first, last = own // TILE, (own + count - 1) // TILE
    ids = lax.broadcasted_iota(jnp.int32, pick.shape, 0) + (first * TILE - own)
    pick[...] = jnp.where(ids == elem[...], live[...], 0.0)
    xp[...] = jnp.zeros(xp.shape, xp.dtype)

    def spread(grp):
        lhs = x[grp]
        res = dot(lhs, wb[0:2 * lanes]) + dot(lhs[:, 0:lanes], wb[2 * lanes:])
        at = slice(grp * TILE, (grp + 1) * TILE)
        shifted = slice(GUARD + grp * TILE, GUARD + (grp + 1) * TILE)
        for f in range(fields):
            part = res[f * TILE:(f + 1) * TILE]
            for k in range(kinds):
                turned[k, f, at] = part[:, k * lanes:(k + 1) * lanes]
            for k in range(2):
                faces[k, f, shifted] = part[:, (kinds + k) * lanes:(kinds + k + 1) * lanes]
            turned[kinds, f, at] = part[:, (kinds + 2) * lanes:]

    def advance(grp):
        top, rows = grp * TILE, TILE
        if grp == 0:
            top, rows = top + margin, rows - margin
        if grp == groups - 1:
            rows = rows - margin
        at = slice(top, top + rows)
        parts = [slice(top + r, top + r + SUB) for r in range(0, rows, SUB)]
        acc = [[None] * fields for _ in parts]
        for k in range(kinds):
            m = [stored(fields + k, top + p * SUB, SUB) for p in range(len(parts))]
            for row in range(fields):
                part_sum = [None] * len(parts)
                for f in range(fields):
                    weight = mixer[(k * fields + row) * fields + f]
                    for p, part in enumerate(parts):
                        term = weight * turned[k, f, part]
                        part_sum[p] = term if f == 0 else part_sum[p] + term
                for p in range(len(parts)):
                    term = part_sum[p] * m[p]
                    acc[p][row] = term if k == 0 else acc[p][row] + term
        acc = [jnp.concatenate(list(rows_of), axis=0) for rows_of in zip(*acc)]
        fresh = []
        for f in range(fields):
            side = faces[0, f, GUARD + top - 1:GUARD + top - 1 + rows] + faces[1, f, GUARD + top + 1:GUARD + top + 1 + rows]
            new = u[f, at] + ((acc[f] + turned[kinds, f, at]) + side)
            if top < own or top + rows > own + count:
                new = new * stored(fields + kinds, top, rows)
            u[f, at] = new
            fresh.append(new)
        if first <= grp <= last:
            hi, lo = split((fresh[3] + fresh[4] + fresh[5]) * (1.0 / 3.0))
            xp[(grp - first) * TILE:(grp - first + 1) * TILE, 0:lanes] = hi
            xp[(grp - first) * TILE:(grp - first + 1) * TILE, lanes:] = lo
        for f in range(fields):
            new = fresh[f]
            if grp == 0:
                new = jnp.concatenate([zeros(margin, lanes), new], axis=0)
            if grp == groups - 1:
                new = jnp.concatenate([new, zeros(margin, lanes)], axis=0)
            put(grp, f, new)

    def sample(t):
        for c in range(COMPS):
            if c < 3:
                lhs = x[first:last + 1, c * TILE:(c + 1) * TILE].reshape(pick.shape[0], 2 * lanes)
            else:
                lhs = xp[...]
            prod = dot(lhs, ws[0:2 * lanes]) + dot(lhs[:, 0:lanes], ws[2 * lanes:])
            rows_out[t, c:c + 1, :] = jnp.sum(prod * pick[...], axis=0, keepdims=True)

    def step(todo, ahead, t, _):
        sample(t)
        for j, grp in enumerate(todo):
            spread(todo[(j + ahead) % len(todo)])
            advance(grp)
        return 0

    for grp in range(AHEAD):
        spread(grp)
    lax.fori_loop(0, WIDE, functools.partial(step, tuple(range(groups)), AHEAD), 0)
    lax.fori_loop(WIDE, STEPS, functools.partial(step, tuple(range(first, last + 1)), AHEAD - 1), 0)
    sample(STEPS)
    out[...] = zeros(*out.shape)
    for c in range(COMPS):
        for t in range(STEPS):
            out[c * STEPS + t:c * STEPS + t + 1, :] = rows_out[t + 1, c:c + 1, :]
    out[COMPS * STEPS:COMPS * STEPS + 1, :] = live[...]


def vm(x):
    return pltpu.with_memory_space_constraint(x, pltpu.VMEM)


VM = pl.BlockSpec(memory_space=pltpu.VMEM)


def shards(initial, derivative, coupling, face_lift, metric, rec_element, rec_weight, live_counts, shot_order, observed):
    fields, nodes, count = initial.shape
    lanes = -(-nodes // 128) * 128
    slots, width = observed.shape
    peers = lax.axis_size("mx")
    span = count + 2 * HALO
    kinds = derivative.shape[0]
    total = span + TILE
    picked = count + TILE
    wide = -(-(width + 1) // 64) * 64
    f32, bf16 = jnp.float32, jnp.bfloat16
    square = pltpu.VMEM((slots, slots), bf16)
    state, wb, ws, to_send, from_send, to_place, from_place, live = pl.pallas_call(
        functools.partial(start_kernel, peers),
        out_shape=(
            pltpu.VMEM((fields + metric.shape[0] + 1, span, lanes), f32),
            pltpu.VMEM((3 * lanes, (kinds + 3) * lanes), bf16),
            pltpu.VMEM((3 * lanes, slots), bf16),
            square, square, square, square,
            pltpu.VMEM((1, slots), f32),
        ),
        in_specs=[VM] * 7,
        out_specs=[VM] * 8,
        scratch_shapes=[
            pltpu.VMEM((lanes, lanes), f32),
            pltpu.VMEM((lanes, slots), f32),
            pltpu.SemaphoreType.DMA((2,)),
            pltpu.SemaphoreType.DMA((2,)),
        ],
        compiler_params=pltpu.CompilerParams(collective_id=0, has_side_effects=True),
        name="start",
    )(initial, metric, derivative, face_lift, rec_weight, shot_order.reshape(peers, slots), live_counts[None, :])
    traces = pl.pallas_call(
        wave_kernel,
        out_shape=pltpu.VMEM((wide, slots), f32),
        in_specs=[VM] * 5 + [pl.BlockSpec(memory_space=pltpu.SMEM)],
        out_specs=VM,
        scratch_shapes=[
            pltpu.VMEM((fields, total, lanes), f32),
            pltpu.VMEM((total // TILE, fields * TILE, 2 * lanes), bf16),
            pltpu.VMEM((picked, 2 * lanes), bf16),
            pltpu.VMEM((kinds + 1, fields, total, lanes), f32),
            pltpu.VMEM((2, fields, total + 2 * GUARD, lanes), f32),
            pltpu.VMEM((picked, slots), f32),
            pltpu.VMEM((STEPS + 1, 8, slots), f32),
            pltpu.VMEM((coupling.size, SUB, lanes), f32),
        ],
        name="waves",
    )(vm(state), vm(wb), vm(ws), rec_element[None, :], vm(live), coupling.reshape(-1))
    residual, misfit, adjoint = pl.pallas_call(
        functools.partial(end_kernel, peers),
        out_shape=(
            pltpu.VMEM((width, slots), f32),
            pltpu.VMEM((1, slots), f32),
            pltpu.VMEM((width, slots), f32),
        ),
        in_specs=[VM] * 6,
        out_specs=[VM] * 3,
        scratch_shapes=[
            pltpu.VMEM((peers, slots // peers, lanes), f32),
            pltpu.VMEM((peers, slots // peers, lanes), f32),
            pltpu.SemaphoreType.DMA((peers,)),
            pltpu.SemaphoreType.DMA((peers,)),
        ],
        compiler_params=pltpu.CompilerParams(collective_id=1, has_side_effects=True),
        name="finish",
    )(vm(traces), observed.T, vm(to_send), vm(from_send), vm(to_place), vm(from_place))
    return residual.T, misfit[0], adjoint.T


def solution(mesh):
    in_specs = (
        P("shots", None, "mx"),
        P(),
        P(),
        P(),
        P(None, "mx"),
        P("mx"),
        P(None, "mx"),
        P(),
        P(),
        P(("shots", "mx"), None),
    )
    out_specs = (P(("shots", "mx"), None), P(("shots", "mx")), P(("shots", "mx"), None))
    return jax.shard_map(shards, mesh=mesh, in_specs=in_specs, out_specs=out_specs, check_vma=False)
```

```python
import functools
import jax
import jax.numpy as jnp
from jax import lax
from jax.experimental import pallas as pl
from jax.experimental.pallas import tpu as pltpu
from jax.sharding import PartitionSpec as P

STEPS = 12
COMPS = 4
HALO = 16
GUARD = 8
TILE = 16
SUB = 8
AHEAD = 3
WIDE = 4
GRANT = 32 * 2 ** 20


def split(x):
    hi = x.astype(jnp.bfloat16)
    return hi, (x - hi.astype(jnp.float32)).astype(jnp.bfloat16)


def zeros(*shape):
    return jnp.zeros(shape, jnp.float32)


def ones_where(cond):
    return jnp.where(cond, 1.0, 0.0).astype(jnp.bfloat16)


def dot(a, b):
    return jnp.dot(a, b, preferred_element_type=jnp.float32)


def permute(onehot, x):
    hi = x.astype(jnp.bfloat16)
    rest = x - hi.astype(jnp.float32)
    mid = rest.astype(jnp.bfloat16)
    low = (rest - mid.astype(jnp.float32)).astype(jnp.bfloat16)
    return dot(onehot, hi) + (dot(onehot, mid) + dot(onehot, low))


def greet(peers, me):
    barrier = pltpu.get_barrier_semaphore()

    def one(off, _):
        pl.semaphore_signal(barrier, inc=1, device_id={"mx": lax.rem(me + off, peers)}, device_id_type=pl.DeviceIdType.MESH)
        return 0

    lax.fori_loop(1, peers, one, 0)
    return barrier


def start_kernel(peers, initial, metric, derivative, face_lift, weight_in, order, counts, elem, coupling,
                 state, wb, ws, to_send, from_send, to_place, from_place, live, mixer, pick,
                 pad, padw, send_sem, recv_sem):
    fields, nodes, count = initial.shape
    lanes = pad.shape[0]
    slots = padw.shape[1]
    pieces = slots // lanes
    pair = slots // peers
    me = lax.axis_index("mx")
    right, left = lax.rem(me + 1, peers), lax.rem(me + peers - 1, peers)
    barrier = pltpu.get_barrier_semaphore()
    for side in (left, right):
        pl.semaphore_signal(barrier, inc=1, device_id={"mx": side}, device_id_type=pl.DeviceIdType.MESH)
    pad[...] = zeros(lanes, lanes)
    for f in range(fields):
        pad[0:nodes, :] = initial[f]
        state[f, HALO:HALO + count] = pad[...].T
    kinds = metric.shape[0]
    for k in range(kinds):
        state[fields + k, HALO:HALO + count] = jnp.broadcast_to(metric[k:k + 1, :], (lanes, count)).T
    pl.semaphore_wait(barrier, 2)
    moved = fields + kinds
    copies = []
    for i, (side, at, to) in enumerate(((right, count, 0), (left, HALO, HALO + count))):
        copies.append(pltpu.make_async_remote_copy(
            src_ref=state.at[0:moved, at:at + HALO], dst_ref=state.at[0:moved, to:to + HALO],
            send_sem=send_sem.at[i], recv_sem=recv_sem.at[i],
            device_id={"mx": side}, device_id_type=pl.DeviceIdType.MESH))
        copies[-1].start()
    pad[...] = zeros(lanes, lanes)
    turns = derivative.shape[0]

    def weigh(k, matrix):
        pad[0:nodes, 0:nodes] = matrix
        hi, lo = split(pad[...].T * (0.5 / STEPS))
        at = slice(k * lanes, (k + 1) * lanes)
        wb[0:lanes, at] = hi
        wb[lanes:2 * lanes, at] = hi
        wb[2 * lanes:, at] = lo

    for k in range(turns):
        weigh(k, derivative[k])
    lower, upper = face_lift[:, 0, :], face_lift[:, 1, :]
    weigh(turns, lower)
    weigh(turns + 1, upper)
    weigh(turns + 2, -(lower + upper))
    padw[...] = zeros(lanes, slots)
    padw[0:nodes, :] = weight_in[...]
    hi, lo = split(padw[...])
    ws[0:lanes] = hi
    ws[lanes:2 * lanes] = hi
    ws[2 * lanes:] = lo
    rows = lax.broadcasted_iota(jnp.int32, (count + 2 * HALO, lanes), 0) + (me * count - HALO)
    state[moved] = jnp.where((rows >= 0) & (rows < count * peers), 1.0, 0.0)

    up = lax.broadcasted_iota(jnp.int32, (slots, slots), 0)
    across = lax.broadcasted_iota(jnp.int32, (slots, slots), 1)
    tri = ones_where(up <= across)
    blocks = jnp.concatenate([order[pl.ds(i, peers, stride=pieces), :] for i in range(pieces)], axis=1)
    source, slot = lax.div(blocks, slots), lax.rem(blocks, slots)
    mine = source == me
    rank = dot(ones_where(mine), tri) - 1.0
    rank = jnp.where(mine, rank, -1.0)
    tall = lax.broadcasted_iota(jnp.int32, (slots, peers), 0)
    wide = lax.broadcasted_iota(jnp.int32, (slots, peers), 1)
    repeat = ones_where(lax.div(tall, pair) == wide)
    rank_all = dot(repeat, rank.astype(jnp.bfloat16))
    slot_all = dot(repeat, slot.astype(jnp.float32).astype(jnp.bfloat16))
    hit = rank_all == lax.rem(up, pair).astype(jnp.float32)
    send_slot = jnp.sum(jnp.where(hit, slot_all, 0.0), axis=1, keepdims=True)
    sends = jnp.where(send_slot == across.astype(jnp.float32), 1.0, 0.0)
    to_send[...] = sends.astype(jnp.bfloat16)
    from_send[...] = sends.T.astype(jnp.bfloat16)
    own = jnp.concatenate([order[pl.ds(me * pieces + i, 1), :] for i in range(pieces)], axis=1)
    own_source = lax.div(own, slots)
    peer_ids = lax.broadcasted_iota(jnp.int32, (peers, slots), 0)
    from_peer = peer_ids == own_source
    seen = dot(ones_where(from_peer), tri) - 1.0
    own_rank = jnp.sum(jnp.where(from_peer, seen, 0.0), axis=0, keepdims=True)
    place = own_source.astype(jnp.float32) * float(pair) + own_rank
    places = jnp.where(up.astype(jnp.float32) == place, 1.0, 0.0)
    to_place[...] = places.astype(jnp.bfloat16)
    from_place[...] = places.T.astype(jnp.bfloat16)
    here = lax.broadcasted_iota(jnp.int32, (1, peers), 1) == me
    limit = jnp.sum(jnp.where(here, counts[...].astype(jnp.float32), 0.0), axis=1, keepdims=True)
    alive = jnp.where(lax.broadcasted_iota(jnp.int32, (1, slots), 1).astype(jnp.float32) < limit, 1.0, 0.0)
    live[...] = alive
    ids = lax.broadcasted_iota(jnp.int32, pick.shape, 0) - (pick.shape[0] - count) // 2
    pick[...] = jnp.where(ids == elem[...], alive, 0.0)
    for row in range(fields):
        for k in range(kinds):
            line = coupling[row, k:k + 1, :]
            for f in range(fields):
                mixer[(k * fields + row) * fields + f] = jnp.broadcast_to(line[:, f:f + 1], (SUB, lanes))
    for copy in copies:
        copy.wait()


def end_kernel(peers, traces, observed, to_send, from_send, to_place, from_place,
               residual, misfit, adjoint, sent, got, send_sem, recv_sem):
    width, slots = observed.shape
    lanes = sent.shape[-1]
    wide = traces.shape[0]
    pair = slots // peers
    me = lax.axis_index("mx")
    barrier = greet(peers, me)
    synth = traces[...].T
    packed = permute(to_send[...], synth)
    a = lax.broadcasted_iota(jnp.int32, (width, width), 0)
    b = lax.broadcasted_iota(jnp.int32, (width, width), 1)
    back = ones_where((lax.div(a, STEPS) == lax.div(b, STEPS)) & (lax.rem(a, STEPS) + lax.rem(b, STEPS) == STEPS - 1))
    obs = permute(to_place[...], permute(back, observed[...]).T)
    row = jnp.concatenate([packed, obs, zeros(slots, lanes - wide - width)], axis=1)
    sent[...] = row.reshape(peers, pair, lanes)
    pl.semaphore_wait(barrier, peers - 1)

    turned = traces[width:width + 1, :] * permute(back, traces[0:width, :])

    def copy_to(off):
        dest = lax.rem(me + off, peers)
        return pltpu.make_async_remote_copy(
            src_ref=sent.at[dest], dst_ref=got.at[me], send_sem=send_sem.at[dest], recv_sem=recv_sem.at[me],
            device_id={"mx": dest}, device_id_type=pl.DeviceIdType.MESH)

    def copy_from(off):
        src = lax.rem(me - off + peers, peers)
        return pltpu.make_async_remote_copy(
            src_ref=sent.at[src], dst_ref=got.at[src], send_sem=send_sem.at[src], recv_sem=recv_sem.at[src],
            device_id={"mx": src}, device_id_type=pl.DeviceIdType.MESH)

    def begin(off, _):
        copy_to(off).start()
        return 0

    def finish(off, _):
        copy_from(off).wait_recv()
        return 0

    def drain(off, _):
        copy_to(off).wait_send()
        return 0

    lax.fori_loop(1, peers, begin, 0)
    got[pl.ds(me, 1)] = sent[pl.ds(me, 1)]
    lax.fori_loop(1, peers, finish, 0)
    arrived = got[...].reshape(slots, lanes)
    placed = permute(from_place[...], arrived[:, :wide]).T
    res = placed[width:width + 1] * (placed[:width] - observed[...])
    residual[...] = res
    misfit[...] = 0.5 * jnp.sum(res * res, axis=0, keepdims=True)
    slot_obs = permute(from_send[...], arrived[:, wide:wide + width]).T
    adjoint[...] = turned - traces[width:width + 1, :] * slot_obs
    lax.fori_loop(1, peers, drain, 0)


def wave_kernel(state, wb, ws, pick, live, mixer, out, u, x, xp, turned, faces, rows_out):
    fields, total, lanes = u.shape
    span = state.shape[1]
    count = span - 2 * HALO
    kinds = turned.shape[0] - 1
    margin = (total - span) // 2
    own = margin + HALO
    slots = ws.shape[1]
    groups = total // TILE

    def stored(f, r, n):
        return state[f, r - margin:r - margin + n]

    def put(grp, f, new):
        hi, lo = split(new)
        x[grp, f * TILE:(f + 1) * TILE, 0:lanes] = hi
        x[grp, f * TILE:(f + 1) * TILE, lanes:] = lo

    for f in range(fields):
        u[f, 0:margin] = zeros(margin, lanes)
        u[f, total - margin:] = zeros(margin, lanes)
        u[f, margin:total - margin] = state[f] * state[fields + kinds]
        for k in range(2):
            faces[k, f, 0:GUARD] = zeros(GUARD, lanes)
            faces[k, f, GUARD + total:] = zeros(GUARD, lanes)
        for grp in range(groups):
            put(grp, f, u[f, grp * TILE:(grp + 1) * TILE])

    first, last = own // TILE, (own + count - 1) // TILE
    xp[...] = jnp.zeros(xp.shape, xp.dtype)

    def spread(grp):
        lhs = x[grp]
        res = dot(lhs, wb[0:2 * lanes]) + dot(lhs[:, 0:lanes], wb[2 * lanes:])
        at = slice(grp * TILE, (grp + 1) * TILE)
        shifted = slice(GUARD + grp * TILE, GUARD + (grp + 1) * TILE)
        for f in range(fields):
            part = res[f * TILE:(f + 1) * TILE]
            for k in range(kinds):
                turned[k, f, at] = part[:, k * lanes:(k + 1) * lanes]
            for k in range(2):
                faces[k, f, shifted] = part[:, (kinds + k) * lanes:(kinds + k + 1) * lanes]
            turned[kinds, f, at] = part[:, (kinds + 2) * lanes:]

    def advance(grp):
        top, rows = grp * TILE, TILE
        if grp == 0:
            top, rows = top + margin, rows - margin
        if grp == groups - 1:
            rows = rows - margin
        at = slice(top, top + rows)
        parts = [slice(top + r, top + r + SUB) for r in range(0, rows, SUB)]
        acc = [[None] * fields for _ in parts]
        for k in range(kinds):
            m = [stored(fields + k, top + p * SUB, SUB) for p in range(len(parts))]
            for row in range(fields):
                part_sum = [None] * len(parts)
                for f in range(fields):
                    weight = mixer[(k * fields + row) * fields + f]
                    for p, part in enumerate(parts):
                        term = weight * turned[k, f, part]
                        part_sum[p] = term if f == 0 else part_sum[p] + term
                for p in range(len(parts)):
                    term = part_sum[p] * m[p]
                    acc[p][row] = term if k == 0 else acc[p][row] + term
        acc = [jnp.concatenate(list(rows_of), axis=0) for rows_of in zip(*acc)]
        fresh = []
        for f in range(fields):
            side = faces[0, f, GUARD + top - 1:GUARD + top - 1 + rows] + faces[1, f, GUARD + top + 1:GUARD + top + 1 + rows]
            new = u[f, at] + ((acc[f] + turned[kinds, f, at]) + side)
            if top < own or top + rows > own + count:
                new = new * stored(fields + kinds, top, rows)
            u[f, at] = new
            fresh.append(new)
        if first <= grp <= last:
            hi, lo = split((fresh[3] + fresh[4] + fresh[5]) * (1.0 / 3.0))
            xp[(grp - first) * TILE:(grp - first + 1) * TILE, 0:lanes] = hi
            xp[(grp - first) * TILE:(grp - first + 1) * TILE, lanes:] = lo
        for f in range(fields):
            new = fresh[f]
            if grp == 0:
                new = jnp.concatenate([zeros(margin, lanes), new], axis=0)
            if grp == groups - 1:
                new = jnp.concatenate([new, zeros(margin, lanes)], axis=0)
            put(grp, f, new)

    def sample(t):
        for c in range(COMPS):
            if c < 3:
                lhs = x[first:last + 1, c * TILE:(c + 1) * TILE].reshape(pick.shape[0], 2 * lanes)
            else:
                lhs = xp[...]
            prod = dot(lhs, ws[0:2 * lanes]) + dot(lhs[:, 0:lanes], ws[2 * lanes:])
            rows_out[t, c:c + 1, :] = jnp.sum(prod * pick[...], axis=0, keepdims=True)

    def step(todo, ahead, t, _):
        sample(t)
        for j, grp in enumerate(todo):
            spread(todo[(j + ahead) % len(todo)])
            advance(grp)
        return 0

    for grp in range(AHEAD):
        spread(grp)
    lax.fori_loop(0, WIDE, functools.partial(step, tuple(range(groups)), AHEAD), 0)
    lax.fori_loop(WIDE, STEPS, functools.partial(step, tuple(range(first, last + 1)), AHEAD - 1), 0)
    sample(STEPS)
    out[...] = zeros(*out.shape)
    for c in range(COMPS):
        for t in range(STEPS):
            out[c * STEPS + t:c * STEPS + t + 1, :] = rows_out[t + 1, c:c + 1, :]
    out[COMPS * STEPS:COMPS * STEPS + 1, :] = live[...]


def vm(x):
    return pltpu.with_memory_space_constraint(x, pltpu.VMEM)


VM = pl.BlockSpec(memory_space=pltpu.VMEM)


def shards(initial, derivative, coupling, face_lift, metric, rec_element, rec_weight, live_counts, shot_order, observed):
    fields, nodes, count = initial.shape
    lanes = -(-nodes // 128) * 128
    slots, width = observed.shape
    peers = lax.axis_size("mx")
    span = count + 2 * HALO
    kinds = derivative.shape[0]
    total = span + TILE
    picked = count + TILE
    wide = -(-(width + 1) // 64) * 64
    f32, bf16 = jnp.float32, jnp.bfloat16
    square = pltpu.VMEM((slots, slots), bf16)
    state, wb, ws, to_send, from_send, to_place, from_place, live, mixer, pick = pl.pallas_call(
        functools.partial(start_kernel, peers),
        out_shape=(
            pltpu.VMEM((fields + metric.shape[0] + 1, span, lanes), f32),
            pltpu.VMEM((3 * lanes, (kinds + 3) * lanes), bf16),
            pltpu.VMEM((3 * lanes, slots), bf16),
            square, square, square, square,
            pltpu.VMEM((1, slots), f32),
            pltpu.VMEM((coupling.size, SUB, lanes), f32),
            pltpu.VMEM((picked, slots), f32),
        ),
        in_specs=[VM] * 9,
        out_specs=[VM] * 10,
        scratch_shapes=[
            pltpu.VMEM((lanes, lanes), f32),
            pltpu.VMEM((lanes, slots), f32),
            pltpu.SemaphoreType.DMA((2,)),
            pltpu.SemaphoreType.DMA((2,)),
        ],
        compiler_params=pltpu.CompilerParams(collective_id=0, has_side_effects=True, vmem_limit_bytes=GRANT),
        name="start",
    )(initial, metric, derivative, face_lift.transpose(1, 0, 2), rec_weight, shot_order.reshape(-1, lanes), live_counts[None, :],
      rec_element[None, :], coupling.transpose(1, 0, 2))
    traces = pl.pallas_call(
        wave_kernel,
        out_shape=pltpu.VMEM((wide, slots), f32),
        in_specs=[VM] * 6,
        out_specs=VM,
        scratch_shapes=[
            pltpu.VMEM((fields, total, lanes), f32),
            pltpu.VMEM((total // TILE, fields * TILE, 2 * lanes), bf16),
            pltpu.VMEM((picked, 2 * lanes), bf16),
            pltpu.VMEM((kinds + 1, fields, total, lanes), f32),
            pltpu.VMEM((2, fields, total + 2 * GUARD, lanes), f32),
            pltpu.VMEM((STEPS + 1, 8, slots), f32),
        ],
        compiler_params=pltpu.CompilerParams(vmem_limit_bytes=GRANT),
        name="waves",
    )(vm(state), vm(wb), vm(ws), vm(pick), vm(live), vm(mixer))
    residual, misfit, adjoint = pl.pallas_call(
        functools.partial(end_kernel, peers),
        out_shape=(
            pltpu.VMEM((width, slots), f32),
            pltpu.VMEM((1, slots), f32),
            pltpu.VMEM((width, slots), f32),
        ),
        in_specs=[VM] * 6,
        out_specs=[VM] * 3,
        scratch_shapes=[
            pltpu.VMEM((peers, slots // peers, lanes), f32),
            pltpu.VMEM((peers, slots // peers, lanes), f32),
            pltpu.SemaphoreType.DMA((peers,)),
            pltpu.SemaphoreType.DMA((peers,)),
        ],
        compiler_params=pltpu.CompilerParams(collective_id=1, has_side_effects=True, vmem_limit_bytes=GRANT),
        name="finish",
    )(vm(traces), observed.T, vm(to_send), vm(from_send), vm(to_place), vm(from_place))
    return residual.T, misfit[0], adjoint.T


def solution(mesh):
    in_specs = (
        P("shots", None, "mx"),
        P(),
        P(),
        P(),
        P(None, "mx"),
        P("mx"),
        P(None, "mx"),
        P(),
        P(),
        P(("shots", "mx"), None),
    )
    out_specs = (P(("shots", "mx"), None), P(("shots", "mx")), P(("shots", "mx"), None))
    return jax.shard_map(shards, mesh=mesh, in_specs=in_specs, out_specs=out_specs, check_vma=False)
```

```python
import functools
import jax
import jax.numpy as jnp
from jax import lax
from jax.experimental import pallas as pl
from jax.experimental.pallas import tpu as pltpu
from jax.sharding import PartitionSpec as P

STEPS = 12
COMPS = 4
HALO = 16
GUARD = 8
TILE = 16
SUB = 8
AHEAD = 3
WIDE = 4
GRANT = 32 * 2 ** 20


def split(x):
    hi = x.astype(jnp.bfloat16)
    return hi, (x - hi.astype(jnp.float32)).astype(jnp.bfloat16)


def zeros(*shape):
    return jnp.zeros(shape, jnp.float32)


def ones_where(cond):
    return jnp.where(cond, 1.0, 0.0).astype(jnp.bfloat16)


def dot(a, b):
    return jnp.dot(a, b, preferred_element_type=jnp.float32)


def permute(onehot, x):
    hi = x.astype(jnp.bfloat16)
    rest = x - hi.astype(jnp.float32)
    mid = rest.astype(jnp.bfloat16)
    low = (rest - mid.astype(jnp.float32)).astype(jnp.bfloat16)
    return dot(onehot, hi) + (dot(onehot, mid) + dot(onehot, low))


def greet(peers, me):
    barrier = pltpu.get_barrier_semaphore()

    def one(off, _):
        pl.semaphore_signal(barrier, inc=1, device_id={"mx": lax.rem(me + off, peers)}, device_id_type=pl.DeviceIdType.MESH)
        return 0

    lax.fori_loop(1, peers, one, 0)
    return barrier


def start_kernel(peers, initial, metric, derivative, face_lift, weight_in, order, counts, elem, coupling,
                 state, wb, ws, to_send, from_send, to_place, from_place, live, mixer, pick,
                 pad, padw, send_sem, recv_sem):
    fields, nodes, count = initial.shape
    lanes = pad.shape[0]
    slots = padw.shape[1]
    pieces = slots // lanes
    pair = slots // peers
    me = lax.axis_index("mx")
    right, left = lax.rem(me + 1, peers), lax.rem(me + peers - 1, peers)
    barrier = pltpu.get_barrier_semaphore()
    for side in (left, right):
        pl.semaphore_signal(barrier, inc=1, device_id={"mx": side}, device_id_type=pl.DeviceIdType.MESH)
    pad[...] = zeros(lanes, lanes)
    for f in range(fields):
        pad[0:nodes, :] = initial[f]
        state[f, HALO:HALO + count] = pad[...].T
    kinds = metric.shape[0]
    for k in range(kinds):
        state[fields + k, HALO:HALO + count] = jnp.broadcast_to(metric[k:k + 1, :], (lanes, count)).T
    pl.semaphore_wait(barrier, 2)
    moved = fields + kinds
    copies = []
    for i, (side, at, to) in enumerate(((right, count, 0), (left, HALO, HALO + count))):
        copies.append(pltpu.make_async_remote_copy(
            src_ref=state.at[0:moved, at:at + HALO], dst_ref=state.at[0:moved, to:to + HALO],
            send_sem=send_sem.at[i], recv_sem=recv_sem.at[i],
            device_id={"mx": side}, device_id_type=pl.DeviceIdType.MESH))
        copies[-1].start()
    pad[...] = zeros(lanes, lanes)
    turns = derivative.shape[0]

    def weigh(k, matrix):
        pad[0:nodes, 0:nodes] = matrix
        hi, lo = split(pad[...].T * (0.5 / STEPS))
        at = slice(k * lanes, (k + 1) * lanes)
        wb[0:lanes, at] = hi
        wb[lanes:2 * lanes, at] = hi
        wb[2 * lanes:, at] = lo

    for k in range(turns):
        weigh(k, derivative[k])
    lower, upper = face_lift[:, 0, :], face_lift[:, 1, :]
    weigh(turns, lower)
    weigh(turns + 1, upper)
    weigh(turns + 2, -(lower + upper))
    padw[...] = zeros(lanes, slots)
    padw[0:nodes, :] = weight_in[...]
    hi, lo = split(padw[...])
    ws[0:lanes] = hi
    ws[lanes:2 * lanes] = hi
    ws[2 * lanes:] = lo
    rows = lax.broadcasted_iota(jnp.int32, (count + 2 * HALO, lanes), 0) + (me * count - HALO)
    state[moved] = jnp.where((rows >= 0) & (rows < count * peers), 1.0, 0.0)

    up = lax.broadcasted_iota(jnp.int32, (slots, slots), 0)
    across = lax.broadcasted_iota(jnp.int32, (slots, slots), 1)
    tri = ones_where(up <= across)
    blocks = jnp.concatenate([order[pl.ds(i, peers, stride=pieces), :] for i in range(pieces)], axis=1)
    source, slot = lax.div(blocks, slots), lax.rem(blocks, slots)
    mine = source == me
    rank = dot(ones_where(mine), tri) - 1.0
    rank = jnp.where(mine, rank, -1.0)
    tall = lax.broadcasted_iota(jnp.int32, (slots, peers), 0)
    wide = lax.broadcasted_iota(jnp.int32, (slots, peers), 1)
    repeat = ones_where(lax.div(tall, pair) == wide)
    rank_all = dot(repeat, rank.astype(jnp.bfloat16))
    slot_all = dot(repeat, slot.astype(jnp.float32).astype(jnp.bfloat16))
    hit = rank_all == lax.rem(up, pair).astype(jnp.float32)
    send_slot = jnp.sum(jnp.where(hit, slot_all, 0.0), axis=1, keepdims=True)
    sends = jnp.where(send_slot == across.astype(jnp.float32), 1.0, 0.0)
    to_send[...] = sends.astype(jnp.bfloat16)
    from_send[...] = sends.T.astype(jnp.bfloat16)
    own = jnp.concatenate([order[pl.ds(me * pieces + i, 1), :] for i in range(pieces)], axis=1)
    own_source = lax.div(own, slots)
    peer_ids = lax.broadcasted_iota(jnp.int32, (peers, slots), 0)
    from_peer = peer_ids == own_source
    seen = dot(ones_where(from_peer), tri) - 1.0
    own_rank = jnp.sum(jnp.where(from_peer, seen, 0.0), axis=0, keepdims=True)
    place = own_source.astype(jnp.float32) * float(pair) + own_rank
    places = jnp.where(up.astype(jnp.float32) == place, 1.0, 0.0)
    to_place[...] = places.astype(jnp.bfloat16)
    from_place[...] = places.T.astype(jnp.bfloat16)
    here = lax.broadcasted_iota(jnp.int32, (1, peers), 1) == me
    limit = jnp.sum(jnp.where(here, counts[...].astype(jnp.float32), 0.0), axis=1, keepdims=True)
    alive = jnp.where(lax.broadcasted_iota(jnp.int32, (1, slots), 1).astype(jnp.float32) < limit, 1.0, 0.0)
    live[...] = alive
    ids = lax.broadcasted_iota(jnp.int32, pick.shape, 0) - (pick.shape[0] - count) // 2
    pick[...] = jnp.where(ids == elem[...], alive, 0.0)
    for row in range(fields):
        for k in range(kinds):
            line = coupling[row, k:k + 1, :]
            for f in range(fields):
                mixer[(k * fields + row) * fields + f] = jnp.broadcast_to(line[:, f:f + 1], (SUB, lanes))
    for copy in copies:
        copy.wait()


def end_kernel(peers, traces, observed, to_send, from_send, to_place, from_place,
               residual, misfit, adjoint, sent, got, send_sem, recv_sem):
    width, slots = observed.shape
    lanes = sent.shape[-1]
    wide = traces.shape[0]
    pair = slots // peers
    me = lax.axis_index("mx")
    barrier = greet(peers, me)
    synth = traces[...].T
    packed = permute(to_send[...], synth)
    a = lax.broadcasted_iota(jnp.int32, (width, width), 0)
    b = lax.broadcasted_iota(jnp.int32, (width, width), 1)
    back = ones_where((lax.div(a, STEPS) == lax.div(b, STEPS)) & (lax.rem(a, STEPS) + lax.rem(b, STEPS) == STEPS - 1))
    obs = permute(to_place[...], permute(back, observed[...]).T)
    row = jnp.concatenate([packed, obs, zeros(slots, lanes - wide - width)], axis=1)
    sent[...] = row.reshape(peers, pair, lanes)
    pl.semaphore_wait(barrier, peers - 1)

    turned = traces[width:width + 1, :] * permute(back, traces[0:width, :])

    def copy_to(off):
        dest = lax.rem(me + off, peers)
        return pltpu.make_async_remote_copy(
            src_ref=sent.at[dest], dst_ref=got.at[me], send_sem=send_sem.at[dest], recv_sem=recv_sem.at[me],
            device_id={"mx": dest}, device_id_type=pl.DeviceIdType.MESH)

    def copy_from(off):
        src = lax.rem(me - off + peers, peers)
        return pltpu.make_async_remote_copy(
            src_ref=sent.at[src], dst_ref=got.at[src], send_sem=send_sem.at[src], recv_sem=recv_sem.at[src],
            device_id={"mx": src}, device_id_type=pl.DeviceIdType.MESH)

    def begin(off, _):
        copy_to(off).start()
        return 0

    def finish(off, _):
        copy_from(off).wait_recv()
        return 0

    def drain(off, _):
        copy_to(off).wait_send()
        return 0

    lax.fori_loop(1, peers, begin, 0)
    got[pl.ds(me, 1)] = sent[pl.ds(me, 1)]
    lax.fori_loop(1, peers, finish, 0)
    arrived = got[...].reshape(slots, lanes)
    placed = permute(from_place[...], arrived[:, :wide]).T
    res = placed[width:width + 1] * (placed[:width] - observed[...])
    residual[...] = res
    misfit[...] = 0.5 * jnp.sum(res * res, axis=0, keepdims=True)
    slot_obs = permute(from_send[...], arrived[:, wide:wide + width]).T
    adjoint[...] = turned - traces[width:width + 1, :] * slot_obs
    lax.fori_loop(1, peers, drain, 0)


def wave_kernel(state, wb_in, ws_in, pick_in, live, mixer_in, out, u, x, xp, turned, faces, rows_out, pick, mixer, wb, ws, held):
    fields, total, lanes = u.shape
    span = state.shape[1]
    count = span - 2 * HALO
    kinds = turned.shape[0] - 1
    margin = (total - span) // 2
    own = margin + HALO
    slots = ws.shape[1]
    groups = total // TILE

    def stored(f, r, n):
        return held[f - fields, r - margin:r - margin + n]

    wb[...] = wb_in[...]
    ws[...] = ws_in[...]
    held[...] = state[fields:]

    def put(grp, f, new):
        hi, lo = split(new)
        x[grp, f * TILE:(f + 1) * TILE, 0:lanes] = hi
        x[grp, f * TILE:(f + 1) * TILE, lanes:] = lo

    for f in range(fields):
        u[f, 0:margin] = zeros(margin, lanes)
        u[f, total - margin:] = zeros(margin, lanes)
        u[f, margin:total - margin] = state[f] * state[fields + kinds]
        for k in range(2):
            faces[k, f, 0:GUARD] = zeros(GUARD, lanes)
            faces[k, f, GUARD + total:] = zeros(GUARD, lanes)
        for grp in range(groups):
            put(grp, f, u[f, grp * TILE:(grp + 1) * TILE])

    first, last = own // TILE, (own + count - 1) // TILE
    xp[...] = jnp.zeros(xp.shape, xp.dtype)
    pick[...] = pick_in[...]
    mixer[...] = mixer_in[...]

    def spread(grp):
        lhs = x[grp]
        res = dot(lhs, wb[0:2 * lanes]) + dot(lhs[:, 0:lanes], wb[2 * lanes:])
        at = slice(grp * TILE, (grp + 1) * TILE)
        shifted = slice(GUARD + grp * TILE, GUARD + (grp + 1) * TILE)
        for f in range(fields):
            part = res[f * TILE:(f + 1) * TILE]
            for k in range(kinds):
                turned[k, f, at] = part[:, k * lanes:(k + 1) * lanes]
            for k in range(2):
                faces[k, f, shifted] = part[:, (kinds + k) * lanes:(kinds + k + 1) * lanes]
            turned[kinds, f, at] = part[:, (kinds + 2) * lanes:]

    def advance(grp):
        top, rows = grp * TILE, TILE
        if grp == 0:
            top, rows = top + margin, rows - margin
        if grp == groups - 1:
            rows = rows - margin
        at = slice(top, top + rows)
        parts = [slice(top + r, top + r + SUB) for r in range(0, rows, SUB)]
        acc = [[None] * fields for _ in parts]
        for k in range(kinds):
            m = [stored(fields + k, top + p * SUB, SUB) for p in range(len(parts))]
            for row in range(fields):
                part_sum = [None] * len(parts)
                for f in range(fields):
                    weight = mixer[(k * fields + row) * fields + f]
                    for p, part in enumerate(parts):
                        term = weight * turned[k, f, part]
                        part_sum[p] = term if f == 0 else part_sum[p] + term
                for p in range(len(parts)):
                    term = part_sum[p] * m[p]
                    acc[p][row] = term if k == 0 else acc[p][row] + term
        acc = [jnp.concatenate(list(rows_of), axis=0) for rows_of in zip(*acc)]
        fresh = []
        for f in range(fields):
            side = faces[0, f, GUARD + top - 1:GUARD + top - 1 + rows] + faces[1, f, GUARD + top + 1:GUARD + top + 1 + rows]
            new = u[f, at] + ((acc[f] + turned[kinds, f, at]) + side)
            if top < own or top + rows > own + count:
                new = new * stored(fields + kinds, top, rows)
            u[f, at] = new
            fresh.append(new)
        if first <= grp <= last:
            hi, lo = split((fresh[3] + fresh[4] + fresh[5]) * (1.0 / 3.0))
            xp[(grp - first) * TILE:(grp - first + 1) * TILE, 0:lanes] = hi
            xp[(grp - first) * TILE:(grp - first + 1) * TILE, lanes:] = lo
        for f in range(fields):
            new = fresh[f]
            if grp == 0:
                new = jnp.concatenate([zeros(margin, lanes), new], axis=0)
            if grp == groups - 1:
                new = jnp.concatenate([new, zeros(margin, lanes)], axis=0)
            put(grp, f, new)

    def sample(t):
        for c in range(COMPS):
            if c < 3:
                lhs = x[first:last + 1, c * TILE:(c + 1) * TILE].reshape(pick.shape[0], 2 * lanes)
            else:
                lhs = xp[...]
            prod = dot(lhs, ws[0:2 * lanes]) + dot(lhs[:, 0:lanes], ws[2 * lanes:])
            rows_out[t, c:c + 1, :] = jnp.sum(prod * pick[...], axis=0, keepdims=True)

    def step(todo, ahead, t, _):
        sample(t)
        for j, grp in enumerate(todo):
            spread(todo[(j + ahead) % len(todo)])
            advance(grp)
        return 0

    for grp in range(AHEAD):
        spread(grp)
    lax.fori_loop(0, WIDE, functools.partial(step, tuple(range(groups)), AHEAD), 0)
    lax.fori_loop(WIDE, STEPS, functools.partial(step, tuple(range(first, last + 1)), AHEAD - 1), 0)
    sample(STEPS)
    out[...] = zeros(*out.shape)
    for c in range(COMPS):
        for t in range(STEPS):
            out[c * STEPS + t:c * STEPS + t + 1, :] = rows_out[t + 1, c:c + 1, :]
    out[COMPS * STEPS:COMPS * STEPS + 1, :] = live[...]


def vm(x):
    return pltpu.with_memory_space_constraint(x, pltpu.VMEM)


def far(x):
    return pltpu.with_memory_space_constraint(x, pltpu.HBM)


VM = pl.BlockSpec(memory_space=pltpu.VMEM)


def shards(initial, derivative, coupling, face_lift, metric, rec_element, rec_weight, live_counts, shot_order, observed):
    fields, nodes, count = initial.shape
    lanes = -(-nodes // 128) * 128
    slots, width = observed.shape
    peers = lax.axis_size("mx")
    span = count + 2 * HALO
    kinds = derivative.shape[0]
    total = span + TILE
    picked = count + TILE
    wide = -(-(width + 1) // 64) * 64
    f32, bf16 = jnp.float32, jnp.bfloat16
    square = pltpu.VMEM((slots, slots), bf16)
    state, wb, ws, to_send, from_send, to_place, from_place, live, mixer, pick = pl.pallas_call(
        functools.partial(start_kernel, peers),
        out_shape=(
            pltpu.VMEM((fields + metric.shape[0] + 1, span, lanes), f32),
            pltpu.VMEM((3 * lanes, (kinds + 3) * lanes), bf16),
            pltpu.VMEM((3 * lanes, slots), bf16),
            square, square, square, square,
            pltpu.VMEM((1, slots), f32),
            pltpu.VMEM((coupling.size, SUB, lanes), f32),
            pltpu.VMEM((picked, slots), f32),
        ),
        in_specs=[VM] * 9,
        out_specs=[VM] * 10,
        scratch_shapes=[
            pltpu.VMEM((lanes, lanes), f32),
            pltpu.VMEM((lanes, slots), f32),
            pltpu.SemaphoreType.DMA((2,)),
            pltpu.SemaphoreType.DMA((2,)),
        ],
        compiler_params=pltpu.CompilerParams(collective_id=0, has_side_effects=True, vmem_limit_bytes=GRANT),
        name="start",
    )(*(far(a) for a in (initial, metric, derivative, face_lift.transpose(1, 0, 2), rec_weight, shot_order.reshape(-1, lanes),
                    live_counts[None, :], rec_element[None, :], coupling.transpose(1, 0, 2))))
    traces = pl.pallas_call(
        wave_kernel,
        out_shape=pltpu.VMEM((wide, slots), f32),
        in_specs=[VM] * 6,
        out_specs=VM,
        scratch_shapes=[
            pltpu.VMEM((fields, total, lanes), f32),
            pltpu.VMEM((total // TILE, fields * TILE, 2 * lanes), bf16),
            pltpu.VMEM((picked, 2 * lanes), bf16),
            pltpu.VMEM((kinds + 1, fields, total, lanes), f32),
            pltpu.VMEM((2, fields, total + 2 * GUARD, lanes), f32),
            pltpu.VMEM((STEPS + 1, 8, slots), f32),
            pltpu.VMEM((picked, slots), f32),
            pltpu.VMEM((coupling.size, SUB, lanes), f32),
            pltpu.VMEM((3 * lanes, (kinds + 3) * lanes), bf16),
            pltpu.VMEM((3 * lanes, slots), bf16),
            pltpu.VMEM((kinds + 1, span, lanes), f32),
        ],
        compiler_params=pltpu.CompilerParams(vmem_limit_bytes=GRANT),
        name="waves",
    )(vm(state), vm(wb), vm(ws), vm(pick), vm(live), vm(mixer))
    residual, misfit, adjoint = pl.pallas_call(
        functools.partial(end_kernel, peers),
        out_shape=(
            pltpu.VMEM((width, slots), f32),
            pltpu.VMEM((1, slots), f32),
            pltpu.VMEM((width, slots), f32),
        ),
        in_specs=[VM] * 6,
        out_specs=[VM] * 3,
        scratch_shapes=[
            pltpu.VMEM((peers, slots // peers, lanes), f32),
            pltpu.VMEM((peers, slots // peers, lanes), f32),
            pltpu.SemaphoreType.DMA((peers,)),
            pltpu.SemaphoreType.DMA((peers,)),
        ],
        compiler_params=pltpu.CompilerParams(collective_id=1, has_side_effects=True, vmem_limit_bytes=GRANT),
        name="finish",
    )(vm(traces), far(observed.T), vm(to_send), vm(from_send), vm(to_place), vm(from_place))
    return residual.T, misfit[0], adjoint.T


def solution(mesh):
    in_specs = (
        P("shots", None, "mx"),
        P(),
        P(),
        P(),
        P(None, "mx"),
        P("mx"),
        P(None, "mx"),
        P(),
        P(),
        P(("shots", "mx"), None),
    )
    out_specs = (P(("shots", "mx"), None), P(("shots", "mx")), P(("shots", "mx"), None))
    return jax.shard_map(shards, mesh=mesh, in_specs=in_specs, out_specs=out_specs, check_vma=False)
```

```python
import functools
import jax
import jax.numpy as jnp
from jax import lax
from jax.experimental import pallas as pl
from jax.experimental.pallas import tpu as pltpu
from jax.sharding import PartitionSpec as P

STEPS = 12
COMPS = 4
HALO = 16
GUARD = 8
TILE = 16
SUB = 8
AHEAD = 3
WIDE = 4
GRANT = 32 * 2 ** 20


def split(x):
    hi = x.astype(jnp.bfloat16)
    return hi, (x - hi.astype(jnp.float32)).astype(jnp.bfloat16)


def zeros(*shape):
    return jnp.zeros(shape, jnp.float32)


def ones_where(cond):
    return jnp.where(cond, 1.0, 0.0).astype(jnp.bfloat16)


def dot(a, b):
    return jnp.dot(a, b, preferred_element_type=jnp.float32)


def permute(onehot, x):
    hi = x.astype(jnp.bfloat16)
    rest = x - hi.astype(jnp.float32)
    mid = rest.astype(jnp.bfloat16)
    low = (rest - mid.astype(jnp.float32)).astype(jnp.bfloat16)
    return dot(onehot, hi) + (dot(onehot, mid) + dot(onehot, low))


def greet(peers, me):
    barrier = pltpu.get_barrier_semaphore()

    def one(off, _):
        pl.semaphore_signal(barrier, inc=1, device_id={"mx": lax.rem(me + off, peers)}, device_id_type=pl.DeviceIdType.MESH)
        return 0

    lax.fori_loop(1, peers, one, 0)
    return barrier


def start_kernel(peers, initial, metric, derivative, face_lift, weight_in, order, counts, elem, coupling,
                 state, wb, ws, to_send, from_send, to_place, from_place, live, mixer, pick,
                 pad, padw, send_sem, recv_sem):
    fields, nodes, count = initial.shape
    lanes = pad.shape[0]
    slots = padw.shape[1]
    pieces = slots // lanes
    pair = slots // peers
    me = lax.axis_index("mx")
    right, left = lax.rem(me + 1, peers), lax.rem(me + peers - 1, peers)
    barrier = pltpu.get_barrier_semaphore()
    sides = ((me < peers - 1, right), (me > 0, left))
    for there, side in sides:
        @pl.when(there)
        def hail():
            pl.semaphore_signal(barrier, inc=1, device_id={"mx": side}, device_id_type=pl.DeviceIdType.MESH)

    pad[...] = zeros(lanes, lanes)
    for f in range(fields):
        pad[0:nodes, :] = initial[f]
        state[f, HALO:HALO + count] = pad[...].T
    kinds = metric.shape[0]
    for k in range(kinds):
        state[fields + k, HALO:HALO + count] = jnp.broadcast_to(metric[k:k + 1, :], (lanes, count)).T
    pl.semaphore_wait(barrier, sum(there.astype(jnp.int32) for there, _ in sides))
    moved = fields + kinds
    copies = []
    for i, (side, at, to) in enumerate(((right, count, 0), (left, HALO, HALO + count))):
        copies.append(pltpu.make_async_remote_copy(
            src_ref=state.at[0:moved, at:at + HALO], dst_ref=state.at[0:moved, to:to + HALO],
            send_sem=send_sem.at[i], recv_sem=recv_sem.at[i],
            device_id={"mx": side}, device_id_type=pl.DeviceIdType.MESH))

    for (there, _), copy, edge in zip(sides, copies, (HALO + count, 0)):
        @pl.when(there)
        def send():
            copy.start()

        @pl.when(jnp.logical_not(there))
        def blank():
            state[0:moved, edge:edge + HALO] = zeros(moved, HALO, lanes)

    pad[...] = zeros(lanes, lanes)
    turns = derivative.shape[0]

    def weigh(k, matrix):
        pad[0:nodes, 0:nodes] = matrix
        hi, lo = split(pad[...].T * (0.5 / STEPS))
        at = slice(k * lanes, (k + 1) * lanes)
        wb[0:lanes, at] = hi
        wb[lanes:2 * lanes, at] = hi
        wb[2 * lanes:, at] = lo

    for k in range(turns):
        weigh(k, derivative[k])
    lower, upper = face_lift[:, 0, :], face_lift[:, 1, :]
    weigh(turns, lower)
    weigh(turns + 1, upper)
    weigh(turns + 2, -(lower + upper))
    padw[...] = zeros(lanes, slots)
    padw[0:nodes, :] = weight_in[...]
    hi, lo = split(padw[...])
    ws[0:lanes] = hi
    ws[lanes:2 * lanes] = hi
    ws[2 * lanes:] = lo
    rows = lax.broadcasted_iota(jnp.int32, (count + 2 * HALO, lanes), 0) + (me * count - HALO)
    state[moved] = jnp.where((rows >= 0) & (rows < count * peers), 1.0, 0.0)

    up = lax.broadcasted_iota(jnp.int32, (slots, slots), 0)
    across = lax.broadcasted_iota(jnp.int32, (slots, slots), 1)
    tri = ones_where(up <= across)
    blocks = jnp.concatenate([order[pl.ds(i, peers, stride=pieces), :] for i in range(pieces)], axis=1)
    source, slot = lax.div(blocks, slots), lax.rem(blocks, slots)
    mine = source == me
    rank = dot(ones_where(mine), tri) - 1.0
    rank = jnp.where(mine, rank, -1.0)
    tall = lax.broadcasted_iota(jnp.int32, (slots, peers), 0)
    wide = lax.broadcasted_iota(jnp.int32, (slots, peers), 1)
    repeat = ones_where(lax.div(tall, pair) == wide)
    rank_all = dot(repeat, rank.astype(jnp.bfloat16))
    slot_all = dot(repeat, slot.astype(jnp.float32).astype(jnp.bfloat16))
    hit = rank_all == lax.rem(up, pair).astype(jnp.float32)
    send_slot = jnp.sum(jnp.where(hit, slot_all, 0.0), axis=1, keepdims=True)
    sends = jnp.where(send_slot == across.astype(jnp.float32), 1.0, 0.0)
    to_send[...] = sends.astype(jnp.bfloat16)
    from_send[...] = sends.T.astype(jnp.bfloat16)
    own = jnp.concatenate([order[pl.ds(me * pieces + i, 1), :] for i in range(pieces)], axis=1)
    own_source = lax.div(own, slots)
    peer_ids = lax.broadcasted_iota(jnp.int32, (peers, slots), 0)
    from_peer = peer_ids == own_source
    seen = dot(ones_where(from_peer), tri) - 1.0
    own_rank = jnp.sum(jnp.where(from_peer, seen, 0.0), axis=0, keepdims=True)
    place = own_source.astype(jnp.float32) * float(pair) + own_rank
    places = jnp.where(up.astype(jnp.float32) == place, 1.0, 0.0)
    to_place[...] = places.astype(jnp.bfloat16)
    from_place[...] = places.T.astype(jnp.bfloat16)
    here = lax.broadcasted_iota(jnp.int32, (1, peers), 1) == me
    limit = jnp.sum(jnp.where(here, counts[...].astype(jnp.float32), 0.0), axis=1, keepdims=True)
    alive = jnp.where(lax.broadcasted_iota(jnp.int32, (1, slots), 1).astype(jnp.float32) < limit, 1.0, 0.0)
    live[...] = alive
    ids = lax.broadcasted_iota(jnp.int32, pick.shape, 0) - (pick.shape[0] - count) // 2
    pick[...] = jnp.where(ids == elem[...], alive, 0.0)
    for row in range(fields):
        for k in range(kinds):
            line = coupling[row, k:k + 1, :]
            for f in range(fields):
                mixer[(k * fields + row) * fields + f] = jnp.broadcast_to(line[:, f:f + 1], (SUB, lanes))
    for (there, _), out, back in zip(sides, copies, copies[::-1]):
        @pl.when(there)
        def finish():
            out.wait_send()
            back.wait_recv()


def whole_kernel(peers, state, wb_in, ws_in, pick_in, live, mixer_in, observed, to_send, from_send, to_place, from_place,
                 residual, misfit, adjoint, u, x, xp, turned, faces, rows_out, pick, mixer, wb, ws, held, traces,
                 sent, got, send_sem, recv_sem):
    width, slots = observed.shape
    lanes = sent.shape[-1]
    wide = traces.shape[0]
    pair = slots // peers
    me = lax.axis_index("mx")
    barrier = greet(peers, me)
    wave_part(state, wb_in, ws_in, pick_in, live, mixer_in, traces, u, x, xp, turned, faces, rows_out, pick, mixer, wb, ws, held)
    synth = traces[...].T
    packed = permute(to_send[...], synth)
    a = lax.broadcasted_iota(jnp.int32, (width, width), 0)
    b = lax.broadcasted_iota(jnp.int32, (width, width), 1)
    back = ones_where((lax.div(a, STEPS) == lax.div(b, STEPS)) & (lax.rem(a, STEPS) + lax.rem(b, STEPS) == STEPS - 1))
    obs = permute(to_place[...], permute(back, observed[...]).T)
    row = jnp.concatenate([packed, obs, zeros(slots, lanes - wide - width)], axis=1)
    sent[...] = row.reshape(peers, pair, lanes)
    pl.semaphore_wait(barrier, peers - 1)

    flipped = traces[width:width + 1, :] * permute(back, traces[0:width, :])

    def copy_to(off):
        dest = lax.rem(me + off, peers)
        return pltpu.make_async_remote_copy(
            src_ref=sent.at[dest], dst_ref=got.at[me], send_sem=send_sem.at[dest], recv_sem=recv_sem.at[me],
            device_id={"mx": dest}, device_id_type=pl.DeviceIdType.MESH)

    def copy_from(off):
        src = lax.rem(me - off + peers, peers)
        return pltpu.make_async_remote_copy(
            src_ref=sent.at[src], dst_ref=got.at[src], send_sem=send_sem.at[src], recv_sem=recv_sem.at[src],
            device_id={"mx": src}, device_id_type=pl.DeviceIdType.MESH)

    def begin(off, _):
        copy_to(off).start()
        return 0

    def finish(off, _):
        copy_from(off).wait_recv()
        return 0

    def drain(off, _):
        copy_to(off).wait_send()
        return 0

    lax.fori_loop(1, peers, begin, 0)
    got[pl.ds(me, 1)] = sent[pl.ds(me, 1)]
    lax.fori_loop(1, peers, finish, 0)
    arrived = got[...].reshape(slots, lanes)
    placed = permute(from_place[...], arrived[:, :wide]).T
    res = placed[width:width + 1] * (placed[:width] - observed[...])
    residual[...] = res
    misfit[...] = 0.5 * jnp.sum(res * res, axis=0, keepdims=True)
    slot_obs = permute(from_send[...], arrived[:, wide:wide + width]).T
    adjoint[...] = flipped - traces[width:width + 1, :] * slot_obs
    lax.fori_loop(1, peers, drain, 0)


def wave_part(state, wb_in, ws_in, pick_in, live, mixer_in, out, u, x, xp, turned, faces, rows_out, pick, mixer, wb, ws, held):
    fields, total, lanes = u.shape
    span = state.shape[1]
    count = span - 2 * HALO
    kinds = turned.shape[0] - 1
    margin = (total - span) // 2
    own = margin + HALO
    slots = ws.shape[1]
    groups = total // TILE

    def stored(f, r, n):
        return held[f - fields, r - margin:r - margin + n]

    wb[...] = wb_in[...]
    ws[...] = ws_in[...]
    held[...] = state[fields:]

    def put(grp, f, new):
        hi, lo = split(new)
        x[grp, f * TILE:(f + 1) * TILE, 0:lanes] = hi
        x[grp, f * TILE:(f + 1) * TILE, lanes:] = lo

    for f in range(fields):
        u[f, 0:margin] = zeros(margin, lanes)
        u[f, total - margin:] = zeros(margin, lanes)
        u[f, margin:total - margin] = state[f] * state[fields + kinds]
        for k in range(2):
            faces[k, f, 0:GUARD] = zeros(GUARD, lanes)
            faces[k, f, GUARD + total:] = zeros(GUARD, lanes)
        for grp in range(groups):
            put(grp, f, u[f, grp * TILE:(grp + 1) * TILE])

    first, last = own // TILE, (own + count - 1) // TILE
    xp[...] = jnp.zeros(xp.shape, xp.dtype)
    pick[...] = pick_in[...]
    mixer[...] = mixer_in[...]

    def spread(grp):
        lhs = x[grp]
        res = dot(lhs, wb[0:2 * lanes]) + dot(lhs[:, 0:lanes], wb[2 * lanes:])
        at = slice(grp * TILE, (grp + 1) * TILE)
        shifted = slice(GUARD + grp * TILE, GUARD + (grp + 1) * TILE)
        for f in range(fields):
            part = res[f * TILE:(f + 1) * TILE]
            for k in range(kinds):
                turned[k, f, at] = part[:, k * lanes:(k + 1) * lanes]
            for k in range(2):
                faces[k, f, shifted] = part[:, (kinds + k) * lanes:(kinds + k + 1) * lanes]
            turned[kinds, f, at] = part[:, (kinds + 2) * lanes:]

    def advance(grp):
        top, rows = grp * TILE, TILE
        if grp == 0:
            top, rows = top + margin, rows - margin
        if grp == groups - 1:
            rows = rows - margin
        at = slice(top, top + rows)
        parts = [slice(top + r, top + r + SUB) for r in range(0, rows, SUB)]
        acc = [[None] * fields for _ in parts]
        for k in range(kinds):
            m = [stored(fields + k, top + p * SUB, SUB) for p in range(len(parts))]
            for row in range(fields):
                part_sum = [None] * len(parts)
                for f in range(fields):
                    weight = mixer[(k * fields + row) * fields + f]
                    for p, part in enumerate(parts):
                        term = weight * turned[k, f, part]
                        part_sum[p] = term if f == 0 else part_sum[p] + term
                for p in range(len(parts)):
                    term = part_sum[p] * m[p]
                    acc[p][row] = term if k == 0 else acc[p][row] + term
        acc = [jnp.concatenate(list(rows_of), axis=0) for rows_of in zip(*acc)]
        fresh = []
        for f in range(fields):
            side = faces[0, f, GUARD + top - 1:GUARD + top - 1 + rows] + faces[1, f, GUARD + top + 1:GUARD + top + 1 + rows]
            new = u[f, at] + ((acc[f] + turned[kinds, f, at]) + side)
            if top < own or top + rows > own + count:
                new = new * stored(fields + kinds, top, rows)
            u[f, at] = new
            fresh.append(new)
        if first <= grp <= last:
            hi, lo = split((fresh[3] + fresh[4] + fresh[5]) * (1.0 / 3.0))
            xp[(grp - first) * TILE:(grp - first + 1) * TILE, 0:lanes] = hi
            xp[(grp - first) * TILE:(grp - first + 1) * TILE, lanes:] = lo
        for f in range(fields):
            new = fresh[f]
            if grp == 0:
                new = jnp.concatenate([zeros(margin, lanes), new], axis=0)
            if grp == groups - 1:
                new = jnp.concatenate([new, zeros(margin, lanes)], axis=0)
            put(grp, f, new)

    def sample(t):
        for c in range(COMPS):
            if c < 3:
                lhs = x[first:last + 1, c * TILE:(c + 1) * TILE].reshape(pick.shape[0], 2 * lanes)
            else:
                lhs = xp[...]
            prod = dot(lhs, ws[0:2 * lanes]) + dot(lhs[:, 0:lanes], ws[2 * lanes:])
            rows_out[t, c:c + 1, :] = jnp.sum(prod * pick[...], axis=0, keepdims=True)

    def step(todo, ahead, t, _):
        sample(t)
        for j, grp in enumerate(todo):
            spread(todo[(j + ahead) % len(todo)])
            advance(grp)
        return 0

    for grp in range(AHEAD):
        spread(grp)
    lax.fori_loop(0, WIDE, functools.partial(step, tuple(range(groups)), AHEAD), 0)
    lax.fori_loop(WIDE, STEPS, functools.partial(step, tuple(range(first, last + 1)), AHEAD - 1), 0)
    sample(STEPS)
    out[...] = zeros(*out.shape)
    for c in range(COMPS):
        for t in range(STEPS):
            out[c * STEPS + t:c * STEPS + t + 1, :] = rows_out[t + 1, c:c + 1, :]
    out[COMPS * STEPS:COMPS * STEPS + 1, :] = live[...]


def vm(x):
    return pltpu.with_memory_space_constraint(x, pltpu.VMEM)


def far(x):
    return pltpu.with_memory_space_constraint(x, pltpu.HBM)


VM = pl.BlockSpec(memory_space=pltpu.VMEM)


def shards(initial, derivative, coupling, face_lift, metric, rec_element, rec_weight, live_counts, shot_order, observed):
    fields, nodes, count = initial.shape
    lanes = -(-nodes // 128) * 128
    slots, width = observed.shape
    peers = lax.axis_size("mx")
    span = count + 2 * HALO
    kinds = derivative.shape[0]
    total = span + TILE
    picked = count + TILE
    wide = -(-(width + 1) // 64) * 64
    f32, bf16 = jnp.float32, jnp.bfloat16
    square = pltpu.VMEM((slots, slots), bf16)
    state, wb, ws, to_send, from_send, to_place, from_place, live, mixer, pick = pl.pallas_call(
        functools.partial(start_kernel, peers),
        out_shape=(
            pltpu.VMEM((fields + metric.shape[0] + 1, span, lanes), f32),
            pltpu.VMEM((3 * lanes, (kinds + 3) * lanes), bf16),
            pltpu.VMEM((3 * lanes, slots), bf16),
            square, square, square, square,
            pltpu.VMEM((1, slots), f32),
            pltpu.VMEM((coupling.size, SUB, lanes), f32),
            pltpu.VMEM((picked, slots), f32),
        ),
        in_specs=[VM] * 9,
        out_specs=[VM] * 10,
        scratch_shapes=[
            pltpu.VMEM((lanes, lanes), f32),
            pltpu.VMEM((lanes, slots), f32),
            pltpu.SemaphoreType.DMA((2,)),
            pltpu.SemaphoreType.DMA((2,)),
        ],
        compiler_params=pltpu.CompilerParams(collective_id=0, has_side_effects=True, vmem_limit_bytes=GRANT),
        name="start",
    )(*(far(a) for a in (initial, metric, derivative, face_lift.transpose(1, 0, 2), rec_weight, shot_order.reshape(-1, lanes),
                    live_counts[None, :], rec_element[None, :], coupling.transpose(1, 0, 2))))
    residual, misfit, adjoint = pl.pallas_call(
        functools.partial(whole_kernel, peers),
        out_shape=(
            pltpu.VMEM((width, slots), f32),
            pltpu.VMEM((1, slots), f32),
            pltpu.VMEM((width, slots), f32),
        ),
        in_specs=[VM] * 11,
        out_specs=[VM] * 3,
        scratch_shapes=[
            pltpu.VMEM((fields, total, lanes), f32),
            pltpu.VMEM((total // TILE, fields * TILE, 2 * lanes), bf16),
            pltpu.VMEM((picked, 2 * lanes), bf16),
            pltpu.VMEM((kinds + 1, fields, total, lanes), f32),
            pltpu.VMEM((2, fields, total + 2 * GUARD, lanes), f32),
            pltpu.VMEM((STEPS + 1, 8, slots), f32),
            pltpu.VMEM((picked, slots), f32),
            pltpu.VMEM((coupling.size, SUB, lanes), f32),
            pltpu.VMEM((3 * lanes, (kinds + 3) * lanes), bf16),
            pltpu.VMEM((3 * lanes, slots), bf16),
            pltpu.VMEM((kinds + 1, span, lanes), f32),
            pltpu.VMEM((wide, slots), f32),
            pltpu.VMEM((peers, slots // peers, lanes), f32),
            pltpu.VMEM((peers, slots // peers, lanes), f32),
            pltpu.SemaphoreType.DMA((peers,)),
            pltpu.SemaphoreType.DMA((peers,)),
        ],
        compiler_params=pltpu.CompilerParams(collective_id=1, has_side_effects=True, vmem_limit_bytes=GRANT),
        name="whole",
    )(vm(state), vm(wb), vm(ws), vm(pick), vm(live), vm(mixer), far(observed.T), vm(to_send), vm(from_send), vm(to_place), vm(from_place))
    return residual.T, misfit[0], adjoint.T


def solution(mesh):
    in_specs = (
        P("shots", None, "mx"),
        P(),
        P(),
        P(),
        P(None, "mx"),
        P("mx"),
        P(None, "mx"),
        P(),
        P(),
        P(("shots", "mx"), None),
    )
    out_specs = (P(("shots", "mx"), None), P(("shots", "mx")), P(("shots", "mx"), None))
    return jax.shard_map(shards, mesh=mesh, in_specs=in_specs, out_specs=out_specs, check_vma=False)
```

```python
import functools
import jax
import jax.numpy as jnp
from jax import lax
from jax.experimental import pallas as pl
from jax.experimental.pallas import tpu as pltpu
from jax.sharding import PartitionSpec as P

STEPS = 12
COMPS = 4
HALO = 16
GUARD = 8
TILE = 16
SUB = 8
AHEAD = 3
WIDE = 4
GRANT = 32 * 2 ** 20


def split(x):
    hi = x.astype(jnp.bfloat16)
    return hi, (x - hi.astype(jnp.float32)).astype(jnp.bfloat16)


def zeros(*shape):
    return jnp.zeros(shape, jnp.float32)


def ones_where(cond):
    return jnp.where(cond, 1.0, 0.0).astype(jnp.bfloat16)


def dot(a, b):
    return jnp.dot(a, b, preferred_element_type=jnp.float32)


def permute(onehot, x):
    hi = x.astype(jnp.bfloat16)
    rest = x - hi.astype(jnp.float32)
    mid = rest.astype(jnp.bfloat16)
    low = (rest - mid.astype(jnp.float32)).astype(jnp.bfloat16)
    return dot(onehot, hi) + (dot(onehot, mid) + dot(onehot, low))


def greet(peers, me):
    barrier = pltpu.get_barrier_semaphore()

    def one(off, _):
        pl.semaphore_signal(barrier, inc=1, device_id={"mx": lax.rem(me + off, peers)}, device_id_type=pl.DeviceIdType.MESH)
        return 0

    lax.fori_loop(1, peers, one, 0)
    return barrier


def start_kernel(peers, initial, metric, derivative, face_lift, weight_in, order, counts, elem, coupling,
                 state, wb, ws, to_send, from_send, to_place, from_place, live, mixer, pick,
                 pad, padw, send_sem, recv_sem):
    fields, nodes, count = initial.shape
    lanes = pad.shape[0]
    slots = padw.shape[1]
    pieces = slots // lanes
    pair = slots // peers
    me = lax.axis_index("mx")
    right, left = lax.rem(me + 1, peers), lax.rem(me + peers - 1, peers)
    barrier = pltpu.get_barrier_semaphore()
    sides = ((me < peers - 1, right), (me > 0, left))
    for there, side in sides:
        @pl.when(there)
        def hail():
            pl.semaphore_signal(barrier, inc=1, device_id={"mx": side}, device_id_type=pl.DeviceIdType.MESH)

    pad[...] = zeros(lanes, lanes)
    for f in range(fields):
        pad[0:nodes, :] = initial[f]
        state[f, HALO:HALO + count] = pad[...].T
    kinds = metric.shape[0]
    for k in range(kinds):
        state[fields + k, HALO:HALO + count] = jnp.broadcast_to(metric[k:k + 1, :], (lanes, count)).T
    pl.semaphore_wait(barrier, sum(there.astype(jnp.int32) for there, _ in sides))
    moved = fields + kinds
    copies = []
    for i, (side, at, to) in enumerate(((right, count, 0), (left, HALO, HALO + count))):
        copies.append(pltpu.make_async_remote_copy(
            src_ref=state.at[0:moved, at:at + HALO], dst_ref=state.at[0:moved, to:to + HALO],
            send_sem=send_sem.at[i], recv_sem=recv_sem.at[i],
            device_id={"mx": side}, device_id_type=pl.DeviceIdType.MESH))

    for (there, _), copy, edge in zip(sides, copies, (HALO + count, 0)):
        @pl.when(there)
        def send():
            copy.start()

        @pl.when(jnp.logical_not(there))
        def blank():
            state[0:moved, edge:edge + HALO] = zeros(moved, HALO, lanes)

    pad[...] = zeros(lanes, lanes)
    turns = derivative.shape[0]

    def weigh(k, matrix):
        pad[0:nodes, 0:nodes] = matrix
        hi, lo = split(pad[...].T * (0.5 / STEPS))
        at = slice(k * lanes, (k + 1) * lanes)
        wb[0:lanes, at] = hi
        wb[lanes:2 * lanes, at] = hi
        wb[2 * lanes:, at] = lo

    for k in range(turns):
        weigh(k, derivative[k])
    below, above = face_lift[:, 0, :], face_lift[:, 1, :]
    weigh(turns, below)
    weigh(turns + 1, above)
    weigh(turns + 2, -(below + above))
    padw[...] = zeros(lanes, slots)
    padw[0:nodes, :] = weight_in[...]
    hi, lo = split(padw[...])
    ws[0:lanes] = hi
    ws[lanes:2 * lanes] = hi
    ws[2 * lanes:] = lo
    rows = lax.broadcasted_iota(jnp.int32, (count + 2 * HALO, lanes), 0) + (me * count - HALO)
    state[moved] = jnp.where((rows >= 0) & (rows < count * peers), 1.0, 0.0)

    up = lax.broadcasted_iota(jnp.int32, (slots, slots), 0)
    across = lax.broadcasted_iota(jnp.int32, (slots, slots), 1)
    tri = ones_where(up <= across)
    blocks = jnp.concatenate([order[pl.ds(i, peers, stride=pieces), :] for i in range(pieces)], axis=1)
    source, slot = lax.div(blocks, slots), lax.rem(blocks, slots)
    mine = source == me
    rank = dot(ones_where(mine), tri) - 1.0
    rank = jnp.where(mine, rank, -1.0)
    tall = lax.broadcasted_iota(jnp.int32, (slots, peers), 0)
    wide = lax.broadcasted_iota(jnp.int32, (slots, peers), 1)
    half, upper = pair // 2, slots // 2
    repeat = ones_where(lax.div(lax.rem(tall, upper), half) == wide)
    rank_all = dot(repeat, rank.astype(jnp.bfloat16))
    slot_all = dot(repeat, slot.astype(jnp.float32).astype(jnp.bfloat16))
    hit = rank_all == (lax.div(up, upper) * half + lax.rem(up, half)).astype(jnp.float32)
    send_slot = jnp.sum(jnp.where(hit, slot_all, 0.0), axis=1, keepdims=True)
    sends = jnp.where(send_slot == across.astype(jnp.float32), 1.0, 0.0)
    to_send[...] = sends.astype(jnp.bfloat16)
    from_send[...] = sends.T.astype(jnp.bfloat16)
    own = jnp.concatenate([order[pl.ds(me * pieces + i, 1), :] for i in range(pieces)], axis=1)
    own_source = lax.div(own, slots)
    peer_ids = lax.broadcasted_iota(jnp.int32, (peers, slots), 0)
    from_peer = peer_ids == own_source
    seen = dot(ones_where(from_peer), tri) - 1.0
    own_rank = jnp.sum(jnp.where(from_peer, seen, 0.0), axis=0, keepdims=True)
    place = own_source.astype(jnp.float32) * float(half) + own_rank + jnp.where(own_rank >= float(half), float(upper - half), 0.0)
    places = jnp.where(up.astype(jnp.float32) == place, 1.0, 0.0)
    to_place[...] = places.astype(jnp.bfloat16)
    from_place[...] = places.T.astype(jnp.bfloat16)
    here = lax.broadcasted_iota(jnp.int32, (1, peers), 1) == me
    limit = jnp.sum(jnp.where(here, counts[...].astype(jnp.float32), 0.0), axis=1, keepdims=True)
    alive = jnp.where(lax.broadcasted_iota(jnp.int32, (1, slots), 1).astype(jnp.float32) < limit, 1.0, 0.0)
    live[...] = alive
    ids = lax.broadcasted_iota(jnp.int32, pick.shape, 0) - (pick.shape[0] - count) // 2
    pick[...] = jnp.where(ids == elem[...], alive, 0.0)
    for row in range(fields):
        for k in range(kinds):
            line = coupling[row, k:k + 1, :]
            for f in range(fields):
                mixer[(k * fields + row) * fields + f] = jnp.broadcast_to(line[:, f:f + 1], (SUB, lanes))
    for (there, _), out, back in zip(sides, copies, copies[::-1]):
        @pl.when(there)
        def finish():
            out.wait_send()
            back.wait_recv()


def fold(rows, peers, lanes):
    slots, wide = rows.shape
    rows = jnp.concatenate([rows[:slots // 2], rows[slots // 2:]], axis=1)
    return rows.reshape(peers, slots // 2 // peers, lanes)


def unfold(block, wide):
    rows = block.reshape(block.shape[0] * block.shape[1], block.shape[2])
    return jnp.concatenate([rows[:, 0:wide], rows[:, wide:]], axis=0)


def whole_kernel(peers, state, wb_in, ws_in, pick_in, live, mixer_in, observed, to_send, from_send, to_place, from_place,
                 outs, u, x, xp, turned, faces, rows_out, pick, mixer, wb, ws, held, traces,
                 sent, got, send_sem, recv_sem):
    width, slots = observed.shape
    residual, misfit, adjoint = outs.at[0:width], outs.at[2 * width:2 * width + 1], outs.at[width:2 * width]
    lanes = sent.shape[-1]
    wide = traces.shape[0]
    me = lax.axis_index("mx")
    barrier = greet(peers, me)
    a = lax.broadcasted_iota(jnp.int32, (width, width), 0)
    b = lax.broadcasted_iota(jnp.int32, (width, width), 1)
    back = ones_where((lax.div(a, STEPS) == lax.div(b, STEPS)) & (lax.rem(a, STEPS) + lax.rem(b, STEPS) == STEPS - 1))
    mirrored = jnp.concatenate([permute(back, observed[...]), zeros(wide - width, slots)], axis=0)
    sent[0] = fold(permute(to_place[...], mirrored.T), peers, lanes)

    def offset(i):
        return 1 + lax.rem(i + peers // 2 - 1, peers - 1)

    def copy_to(which, i):
        dest = lax.rem(me + offset(i), peers)
        return pltpu.make_async_remote_copy(
            src_ref=sent.at[which, dest], dst_ref=got.at[which, me],
            send_sem=send_sem.at[which, dest], recv_sem=recv_sem.at[which, me],
            device_id={"mx": dest}, device_id_type=pl.DeviceIdType.MESH)

    def copy_from(which, i):
        src = lax.rem(me - offset(i) + peers, peers)
        return pltpu.make_async_remote_copy(
            src_ref=sent.at[which, src], dst_ref=got.at[which, src],
            send_sem=send_sem.at[which, src], recv_sem=recv_sem.at[which, src],
            device_id={"mx": src}, device_id_type=pl.DeviceIdType.MESH)

    def begin(which, i, _):
        copy_to(which, i).start()
        return 0

    def finish(which, i, _):
        copy_from(which, i).wait_recv()
        return 0

    def drain(which, i, _):
        copy_to(which, i).wait_send()
        return 0

    def each(action, which):
        lax.fori_loop(0, peers - 1, functools.partial(action, which), 0)

    def between():
        pl.semaphore_wait(barrier, peers - 1)
        each(begin, 0)
        got[0, pl.ds(me, 1)] = sent[0, pl.ds(me, 1)]

    wave_part(between, state, wb_in, ws_in, pick_in, live, mixer_in, traces, u, x, xp, turned, faces, rows_out, pick, mixer, wb, ws, held)
    sent[1] = fold(permute(to_send[...], traces[...].T), peers, lanes)
    each(begin, 1)
    got[1, pl.ds(me, 1)] = sent[1, pl.ds(me, 1)]
    each(finish, 0)
    slot_obs = permute(from_send[...], unfold(got[0], wide)).T
    mine = traces[width:width + 1, :]
    adjoint[...] = mine * (permute(back, traces[0:width, :]) - slot_obs[0:width])
    each(drain, 0)
    each(finish, 1)
    placed = permute(from_place[...], unfold(got[1], wide)).T
    res = placed[width:width + 1] * (placed[:width] - observed[...])
    residual[...] = res
    misfit[...] = 0.5 * jnp.sum(res * res, axis=0, keepdims=True)
    each(drain, 1)


def wave_part(between, state, wb_in, ws_in, pick_in, live, mixer_in, out, u, x, xp, turned, faces, rows_out, pick, mixer, wb, ws, held):
    fields, total, lanes = u.shape
    span = state.shape[1]
    count = span - 2 * HALO
    kinds = turned.shape[0] - 1
    margin = (total - span) // 2
    own = margin + HALO
    slots = ws.shape[1]
    groups = total // TILE

    def stored(f, r, n):
        return held[f - fields, r - margin:r - margin + n]

    wb[...] = wb_in[...]
    ws[...] = ws_in[...]
    held[...] = state[fields:]

    def put(grp, f, new):
        hi, lo = split(new)
        x[grp, f * TILE:(f + 1) * TILE, 0:lanes] = hi
        x[grp, f * TILE:(f + 1) * TILE, lanes:] = lo

    for f in range(fields):
        u[f, 0:margin] = zeros(margin, lanes)
        u[f, total - margin:] = zeros(margin, lanes)
        u[f, margin:total - margin] = state[f] * state[fields + kinds]
        for k in range(2):
            faces[k, f, 0:GUARD] = zeros(GUARD, lanes)
            faces[k, f, GUARD + total:] = zeros(GUARD, lanes)
        for grp in range(groups):
            put(grp, f, u[f, grp * TILE:(grp + 1) * TILE])

    first, last = own // TILE, (own + count - 1) // TILE
    xp[...] = jnp.zeros(xp.shape, xp.dtype)
    pick[...] = pick_in[...]
    mixer[...] = mixer_in[...]

    def spread(grp):
        lhs = x[grp]
        res = dot(lhs, wb[0:2 * lanes]) + dot(lhs[:, 0:lanes], wb[2 * lanes:])
        at = slice(grp * TILE, (grp + 1) * TILE)
        shifted = slice(GUARD + grp * TILE, GUARD + (grp + 1) * TILE)
        for f in range(fields):
            part = res[f * TILE:(f + 1) * TILE]
            for k in range(kinds):
                turned[k, f, at] = part[:, k * lanes:(k + 1) * lanes]
            for k in range(2):
                faces[k, f, shifted] = part[:, (kinds + k) * lanes:(kinds + k + 1) * lanes]
            turned[kinds, f, at] = part[:, (kinds + 2) * lanes:]

    def advance(grp):
        top, rows = grp * TILE, TILE
        if grp == 0:
            top, rows = top + margin, rows - margin
        if grp == groups - 1:
            rows = rows - margin
        at = slice(top, top + rows)
        parts = [slice(top + r, top + r + SUB) for r in range(0, rows, SUB)]
        acc = [[None] * fields for _ in parts]
        for k in range(kinds):
            m = [stored(fields + k, top + p * SUB, SUB) for p in range(len(parts))]
            for row in range(fields):
                part_sum = [None] * len(parts)
                for f in range(fields):
                    weight = mixer[(k * fields + row) * fields + f]
                    for p, part in enumerate(parts):
                        term = weight * turned[k, f, part]
                        part_sum[p] = term if f == 0 else part_sum[p] + term
                for p in range(len(parts)):
                    term = part_sum[p] * m[p]
                    acc[p][row] = term if k == 0 else acc[p][row] + term
        acc = [jnp.concatenate(list(rows_of), axis=0) for rows_of in zip(*acc)]
        fresh = []
        for f in range(fields):
            side = faces[0, f, GUARD + top - 1:GUARD + top - 1 + rows] + faces[1, f, GUARD + top + 1:GUARD + top + 1 + rows]
            new = u[f, at] + ((acc[f] + turned[kinds, f, at]) + side)
            if top < own or top + rows > own + count:
                new = new * stored(fields + kinds, top, rows)
            u[f, at] = new
            fresh.append(new)
        if first <= grp <= last:
            hi, lo = split((fresh[3] + fresh[4] + fresh[5]) * (1.0 / 3.0))
            xp[(grp - first) * TILE:(grp - first + 1) * TILE, 0:lanes] = hi
            xp[(grp - first) * TILE:(grp - first + 1) * TILE, lanes:] = lo
        for f in range(fields):
            new = fresh[f]
            if grp == 0:
                new = jnp.concatenate([zeros(margin, lanes), new], axis=0)
            if grp == groups - 1:
                new = jnp.concatenate([new, zeros(margin, lanes)], axis=0)
            put(grp, f, new)

    def sample(t):
        for c in range(COMPS):
            if c < 3:
                lhs = x[first:last + 1, c * TILE:(c + 1) * TILE].reshape(pick.shape[0], 2 * lanes)
            else:
                lhs = xp[...]
            prod = dot(lhs, ws[0:2 * lanes]) + dot(lhs[:, 0:lanes], ws[2 * lanes:])
            rows_out[t, c:c + 1, :] = jnp.sum(prod * pick[...], axis=0, keepdims=True)

    def step(todo, ahead, t, _):
        sample(t)
        for j, grp in enumerate(todo):
            spread(todo[(j + ahead) % len(todo)])
            advance(grp)
        return 0

    for grp in range(AHEAD):
        spread(grp)
    lax.fori_loop(0, WIDE, functools.partial(step, tuple(range(groups)), AHEAD), 0)
    between()
    lax.fori_loop(WIDE, STEPS, functools.partial(step, tuple(range(first, last + 1)), AHEAD - 1), 0)
    sample(STEPS)
    out[...] = zeros(*out.shape)
    for c in range(COMPS):
        for t in range(STEPS):
            out[c * STEPS + t:c * STEPS + t + 1, :] = rows_out[t + 1, c:c + 1, :]
    out[COMPS * STEPS:COMPS * STEPS + 1, :] = live[...]


def vm(x):
    return pltpu.with_memory_space_constraint(x, pltpu.VMEM)


def far(x):
    return pltpu.with_memory_space_constraint(x, pltpu.HBM)


VM = pl.BlockSpec(memory_space=pltpu.VMEM)


def shards(initial, derivative, coupling, face_lift, metric, rec_element, rec_weight, live_counts, shot_order, observed):
    fields, nodes, count = initial.shape
    lanes = -(-nodes // 128) * 128
    slots, width = observed.shape
    peers = lax.axis_size("mx")
    span = count + 2 * HALO
    kinds = derivative.shape[0]
    total = span + TILE
    picked = count + TILE
    wide = -(-(width + 1) // 64) * 64
    f32, bf16 = jnp.float32, jnp.bfloat16
    square = pltpu.VMEM((slots, slots), bf16)
    state, wb, ws, to_send, from_send, to_place, from_place, live, mixer, pick = pl.pallas_call(
        functools.partial(start_kernel, peers),
        out_shape=(
            pltpu.VMEM((fields + metric.shape[0] + 1, span, lanes), f32),
            pltpu.VMEM((3 * lanes, (kinds + 3) * lanes), bf16),
            pltpu.VMEM((3 * lanes, slots), bf16),
            square, square, square, square,
            pltpu.VMEM((1, slots), f32),
            pltpu.VMEM((coupling.size, SUB, lanes), f32),
            pltpu.VMEM((picked, slots), f32),
        ),
        in_specs=[VM] * 9,
        out_specs=[VM] * 10,
        scratch_shapes=[
            pltpu.VMEM((lanes, lanes), f32),
            pltpu.VMEM((lanes, slots), f32),
            pltpu.SemaphoreType.DMA((2,)),
            pltpu.SemaphoreType.DMA((2,)),
        ],
        compiler_params=pltpu.CompilerParams(collective_id=0, has_side_effects=True, vmem_limit_bytes=GRANT),
        name="start",
    )(*(far(a) for a in (initial, metric, derivative, face_lift.transpose(1, 0, 2), rec_weight, shot_order.reshape(-1, lanes),
                    live_counts[None, :], rec_element[None, :], coupling.transpose(1, 0, 2))))
    out, = pl.pallas_call(
        functools.partial(whole_kernel, peers),
        out_shape=(
            pltpu.VMEM((2 * width + 8, slots), f32),
        ),
        in_specs=[VM] * 11,
        out_specs=[VM],
        scratch_shapes=[
            pltpu.VMEM((fields, total, lanes), f32),
            pltpu.VMEM((total // TILE, fields * TILE, 2 * lanes), bf16),
            pltpu.VMEM((picked, 2 * lanes), bf16),
            pltpu.VMEM((kinds + 1, fields, total, lanes), f32),
            pltpu.VMEM((2, fields, total + 2 * GUARD, lanes), f32),
            pltpu.VMEM((STEPS + 1, 8, slots), f32),
            pltpu.VMEM((picked, slots), f32),
            pltpu.VMEM((coupling.size, SUB, lanes), f32),
            pltpu.VMEM((3 * lanes, (kinds + 3) * lanes), bf16),
            pltpu.VMEM((3 * lanes, slots), bf16),
            pltpu.VMEM((kinds + 1, span, lanes), f32),
            pltpu.VMEM((wide, slots), f32),
            pltpu.VMEM((2, peers, slots // peers // 2, lanes), f32),
            pltpu.VMEM((2, peers, slots // peers // 2, lanes), f32),
            pltpu.SemaphoreType.DMA((2, peers)),
            pltpu.SemaphoreType.DMA((2, peers)),
        ],
        compiler_params=pltpu.CompilerParams(collective_id=1, has_side_effects=True, vmem_limit_bytes=GRANT),
        name="whole",
    )(vm(state), vm(wb), vm(ws), vm(pick), vm(live), vm(mixer), far(observed.T), vm(to_send), vm(from_send), vm(to_place), vm(from_place))
    return out[:width].T, out[2 * width], out[width:2 * width].T


def solution(mesh):
    in_specs = (
        P("shots", None, "mx"),
        P(),
        P(),
        P(),
        P(None, "mx"),
        P("mx"),
        P(None, "mx"),
        P(),
        P(),
        P(("shots", "mx"), None),
    )
    out_specs = (P(("shots", "mx"), None), P(("shots", "mx")), P(("shots", "mx"), None))
    return jax.shard_map(shards, mesh=mesh, in_specs=in_specs, out_specs=out_specs, check_vma=False)
```

```python
import functools
import jax
import jax.numpy as jnp
from jax import lax
from jax.experimental import pallas as pl
from jax.experimental.pallas import tpu as pltpu
from jax.sharding import PartitionSpec as P

STEPS = 12
COMPS = 4
HALO = 16
REACH = 12
GUARD = 8
TILE = 16
SUB = 8
AHEAD = 3
WIDE = 4
GRANT = 32 * 2 ** 20


def split(x):
    hi = x.astype(jnp.bfloat16)
    return hi, (x - hi.astype(jnp.float32)).astype(jnp.bfloat16)


def zeros(*shape):
    return jnp.zeros(shape, jnp.float32)


def ones_where(cond):
    return jnp.where(cond, 1.0, 0.0).astype(jnp.bfloat16)


def dot(a, b):
    return jnp.dot(a, b, preferred_element_type=jnp.float32)


def permute(onehot, x):
    hi = x.astype(jnp.bfloat16)
    rest = x - hi.astype(jnp.float32)
    mid = rest.astype(jnp.bfloat16)
    low = (rest - mid.astype(jnp.float32)).astype(jnp.bfloat16)
    return dot(onehot, hi) + (dot(onehot, mid) + dot(onehot, low))


def greet(peers, me):
    barrier = pltpu.get_barrier_semaphore()

    def one(off, _):
        pl.semaphore_signal(barrier, inc=1, device_id={"mx": lax.rem(me + off, peers)}, device_id_type=pl.DeviceIdType.MESH)
        return 0

    lax.fori_loop(1, peers, one, 0)
    return barrier


def mirror(width):
    a = lax.broadcasted_iota(jnp.int32, (width, width), 0)
    b = lax.broadcasted_iota(jnp.int32, (width, width), 1)
    return ones_where((lax.div(a, STEPS) == lax.div(b, STEPS)) & (lax.rem(a, STEPS) + lax.rem(b, STEPS) == STEPS - 1))


def fold(rows, peers, lanes):
    slots, wide = rows.shape
    rows = jnp.concatenate([rows[:slots // 2], rows[slots // 2:]], axis=1)
    return rows.reshape(peers, slots // 2 // peers, lanes)


def start_kernel(peers, initial, metric, derivative, face_lift, weight_in, order, counts, elem, coupling, observed,
                 state, wb, ws, to_send, from_send, told, from_place, live, mixer, pick,
                 pad, padw, send_sem, recv_sem):
    fields, nodes, count = initial.shape
    lanes = pad.shape[0]
    slots = padw.shape[1]
    pieces = slots // lanes
    pair = slots // peers
    me = lax.axis_index("mx")
    right, left = lax.rem(me + 1, peers), lax.rem(me + peers - 1, peers)
    barrier = pltpu.get_barrier_semaphore()
    sides = ((me < peers - 1, right), (me > 0, left))
    for there, side in sides:
        @pl.when(there)
        def hail():
            pl.semaphore_signal(barrier, inc=1, device_id={"mx": side}, device_id_type=pl.DeviceIdType.MESH)

    pad[...] = zeros(lanes, lanes)
    for f in range(fields):
        pad[0:nodes, :] = initial[f]
        state[f, HALO:HALO + count] = pad[...].T
    kinds = metric.shape[0]
    for k in range(kinds):
        state[fields + k, HALO:HALO + count] = jnp.broadcast_to(metric[k:k + 1, :], (lanes, count)).T
    pl.semaphore_wait(barrier, sum(there.astype(jnp.int32) for there, _ in sides))
    moved = fields + kinds
    copies = []
    for i, (side, at, to) in enumerate(((right, HALO + count - REACH, HALO - REACH), (left, HALO, HALO + count))):
        copies.append(pltpu.make_async_remote_copy(
            src_ref=state.at[0:moved, at:at + REACH], dst_ref=state.at[0:moved, to:to + REACH],
            send_sem=send_sem.at[i], recv_sem=recv_sem.at[i],
            device_id={"mx": side}, device_id_type=pl.DeviceIdType.MESH))

    state[0:moved, 0:HALO - REACH] = zeros(moved, HALO - REACH, lanes)
    state[0:moved, HALO + count + REACH:] = zeros(moved, HALO - REACH, lanes)
    for (there, _), copy, edge in zip(sides, copies, (HALO + count, HALO - REACH)):
        @pl.when(there)
        def send():
            copy.start()

        @pl.when(jnp.logical_not(there))
        def blank():
            state[0:moved, edge:edge + REACH] = zeros(moved, REACH, lanes)

    pad[...] = zeros(lanes, lanes)
    turns = derivative.shape[0]

    def weigh(k, matrix):
        pad[0:nodes, 0:nodes] = matrix
        hi, lo = split(pad[...].T * (0.5 / STEPS))
        at = slice(k * lanes, (k + 1) * lanes)
        wb[0:lanes, at] = hi
        wb[lanes:2 * lanes, at] = hi
        wb[2 * lanes:, at] = lo

    for k in range(turns):
        weigh(k, derivative[k])
    below, above = face_lift[:, 0, :], face_lift[:, 1, :]
    weigh(turns, below)
    weigh(turns + 1, above)
    weigh(turns + 2, -(below + above))
    padw[...] = zeros(lanes, slots)
    padw[0:nodes, :] = weight_in[...]
    hi, lo = split(padw[...])
    ws[0:lanes] = hi
    ws[lanes:2 * lanes] = hi
    ws[2 * lanes:] = lo
    rows = lax.broadcasted_iota(jnp.int32, (count + 2 * HALO, lanes), 0) + (me * count - HALO)
    state[moved] = jnp.where((rows >= 0) & (rows < count * peers), 1.0, 0.0)

    up = lax.broadcasted_iota(jnp.int32, (slots, slots), 0)
    across = lax.broadcasted_iota(jnp.int32, (slots, slots), 1)
    tri = ones_where(up <= across)
    blocks = jnp.concatenate([order[pl.ds(i, peers, stride=pieces), :] for i in range(pieces)], axis=1)
    source, slot = lax.div(blocks, slots), lax.rem(blocks, slots)
    mine = source == me
    rank = dot(ones_where(mine), tri) - 1.0
    rank = jnp.where(mine, rank, -1.0)
    tall = lax.broadcasted_iota(jnp.int32, (slots, peers), 0)
    wide = lax.broadcasted_iota(jnp.int32, (slots, peers), 1)
    half, upper = pair // 2, slots // 2
    repeat = ones_where(lax.div(lax.rem(tall, upper), half) == wide)
    rank_all = dot(repeat, rank.astype(jnp.bfloat16))
    slot_all = dot(repeat, slot.astype(jnp.float32).astype(jnp.bfloat16))
    hit = rank_all == (lax.div(up, upper) * half + lax.rem(up, half)).astype(jnp.float32)
    send_slot = jnp.sum(jnp.where(hit, slot_all, 0.0), axis=1, keepdims=True)
    sends = jnp.where(send_slot == across.astype(jnp.float32), 1.0, 0.0)
    to_send[...] = sends.astype(jnp.bfloat16)
    from_send[...] = sends.T.astype(jnp.bfloat16)
    own = jnp.concatenate([order[pl.ds(me * pieces + i, 1), :] for i in range(pieces)], axis=1)
    own_source = lax.div(own, slots)
    peer_ids = lax.broadcasted_iota(jnp.int32, (peers, slots), 0)
    from_peer = peer_ids == own_source
    seen = dot(ones_where(from_peer), tri) - 1.0
    own_rank = jnp.sum(jnp.where(from_peer, seen, 0.0), axis=0, keepdims=True)
    place = own_source.astype(jnp.float32) * float(half) + own_rank + jnp.where(own_rank >= float(half), float(upper - half), 0.0)
    places = jnp.where(up.astype(jnp.float32) == place, 1.0, 0.0)
    width = observed.shape[0]
    mirrored = jnp.concatenate([permute(mirror(width), observed[...]), zeros(lanes // 2 - width, slots)], axis=0)
    told[...] = fold(permute(places.astype(jnp.bfloat16), mirrored.T), peers, lanes)
    from_place[...] = places.T.astype(jnp.bfloat16)
    here = lax.broadcasted_iota(jnp.int32, (1, peers), 1) == me
    limit = jnp.sum(jnp.where(here, counts[...].astype(jnp.float32), 0.0), axis=1, keepdims=True)
    alive = jnp.where(lax.broadcasted_iota(jnp.int32, (1, slots), 1).astype(jnp.float32) < limit, 1.0, 0.0)
    live[...] = alive
    ids = lax.broadcasted_iota(jnp.int32, pick.shape, 0) - (pick.shape[0] - count) // 2
    pick[...] = jnp.where(ids == elem[...], alive, 0.0)
    for row in range(fields):
        for k in range(kinds):
            line = coupling[row, k:k + 1, :]
            for f in range(fields):
                mixer[(k * fields + row) * fields + f] = jnp.broadcast_to(line[:, f:f + 1], (SUB, lanes))
    for (there, _), out, back in zip(sides, copies, copies[::-1]):
        @pl.when(there)
        def finish():
            out.wait_send()
            back.wait_recv()


def unfold(block, wide):
    rows = block.reshape(block.shape[0] * block.shape[1], block.shape[2])
    return jnp.concatenate([rows[:, 0:wide], rows[:, wide:]], axis=0)


def whole_kernel(peers, state, wb_in, ws_in, pick_in, live, mixer_in, observed, to_send, from_send, told, from_place,
                 outs, u, x, xp, turned, faces, rows_out, pick, mixer, wb, ws, held, traces,
                 sent, got, send_sem, recv_sem):
    width, slots = observed.shape
    residual, misfit, adjoint = outs.at[0:width], outs.at[2 * width:2 * width + 1], outs.at[width:2 * width]
    lanes = sent.shape[-1]
    wide = traces.shape[0]
    me = lax.axis_index("mx")
    barrier = greet(peers, me)
    sent[0] = told[...]
    back = mirror(width)

    def offset(i):
        return 1 + lax.rem(i + peers // 2 - 1, peers - 1)

    def copy_to(which, i):
        dest = lax.rem(me + offset(i), peers)
        return pltpu.make_async_remote_copy(
            src_ref=sent.at[which, dest], dst_ref=got.at[which, me],
            send_sem=send_sem.at[which, dest], recv_sem=recv_sem.at[which, me],
            device_id={"mx": dest}, device_id_type=pl.DeviceIdType.MESH)

    def copy_from(which, i):
        src = lax.rem(me - offset(i) + peers, peers)
        return pltpu.make_async_remote_copy(
            src_ref=sent.at[which, src], dst_ref=got.at[which, src],
            send_sem=send_sem.at[which, src], recv_sem=recv_sem.at[which, src],
            device_id={"mx": src}, device_id_type=pl.DeviceIdType.MESH)

    def begin(which, i, _):
        copy_to(which, i).start()
        return 0

    def finish(which, i, _):
        copy_from(which, i).wait_recv()
        return 0

    def drain(which, i, _):
        copy_to(which, i).wait_send()
        return 0

    def each(action, which):
        lax.fori_loop(0, peers - 1, functools.partial(action, which), 0)

    def between():
        pl.semaphore_wait(barrier, peers - 1)
        each(begin, 0)
        got[0, pl.ds(me, 1)] = sent[0, pl.ds(me, 1)]

    wave_part(between, state, wb_in, ws_in, pick_in, live, mixer_in, traces, u, x, xp, turned, faces, rows_out, pick, mixer, wb, ws, held)
    sent[1] = fold(permute(to_send[...], traces[...].T), peers, lanes)
    each(begin, 1)
    got[1, pl.ds(me, 1)] = sent[1, pl.ds(me, 1)]
    each(finish, 0)
    slot_obs = permute(from_send[...], unfold(got[0], wide)).T
    mine = traces[width:width + 1, :]
    adjoint[...] = mine * (permute(back, traces[0:width, :]) - slot_obs[0:width])
    each(drain, 0)
    each(finish, 1)
    placed = permute(from_place[...], unfold(got[1], wide)).T
    res = placed[width:width + 1] * (placed[:width] - observed[...])
    residual[...] = res
    misfit[...] = 0.5 * jnp.sum(res * res, axis=0, keepdims=True)
    each(drain, 1)


def wave_part(between, state, wb_in, ws_in, pick_in, live, mixer_in, out, u, x, xp, turned, faces, rows_out, pick, mixer, wb, ws, held):
    fields, total, lanes = u.shape
    span = state.shape[1]
    count = span - 2 * HALO
    kinds = turned.shape[0] - 1
    margin = (total - span) // 2
    own = margin + HALO
    slots = ws.shape[1]
    groups = total // TILE

    def stored(f, r, n):
        return held[f - fields, r - margin:r - margin + n]

    wb[...] = wb_in[...]
    ws[...] = ws_in[...]
    held[...] = state[fields:]

    def put(grp, f, new):
        hi, lo = split(new)
        x[grp, f * TILE:(f + 1) * TILE, 0:lanes] = hi
        x[grp, f * TILE:(f + 1) * TILE, lanes:] = lo

    for f in range(fields):
        u[f, 0:margin] = zeros(margin, lanes)
        u[f, total - margin:] = zeros(margin, lanes)
        u[f, margin:total - margin] = state[f] * state[fields + kinds]
        for k in range(2):
            faces[k, f, 0:GUARD] = zeros(GUARD, lanes)
            faces[k, f, GUARD + total:] = zeros(GUARD, lanes)
        for grp in range(groups):
            put(grp, f, u[f, grp * TILE:(grp + 1) * TILE])

    first, last = own // TILE, (own + count - 1) // TILE
    xp[...] = jnp.zeros(xp.shape, xp.dtype)
    pick[...] = pick_in[...]
    mixer[...] = mixer_in[...]

    def spread(grp):
        lhs = x[grp]
        res = dot(lhs, wb[0:2 * lanes]) + dot(lhs[:, 0:lanes], wb[2 * lanes:])
        at = slice(grp * TILE, (grp + 1) * TILE)
        shifted = slice(GUARD + grp * TILE, GUARD + (grp + 1) * TILE)
        for f in range(fields):
            part = res[f * TILE:(f + 1) * TILE]
            for k in range(kinds):
                turned[k, f, at] = part[:, k * lanes:(k + 1) * lanes]
            for k in range(2):
                faces[k, f, shifted] = part[:, (kinds + k) * lanes:(kinds + k + 1) * lanes]
            turned[kinds, f, at] = part[:, (kinds + 2) * lanes:]

    def advance(grp):
        top, rows = grp * TILE, TILE
        if grp == 0:
            top, rows = top + margin, rows - margin
        if grp == groups - 1:
            rows = rows - margin
        at = slice(top, top + rows)
        parts = [slice(top + r, top + r + SUB) for r in range(0, rows, SUB)]
        acc = [[None] * fields for _ in parts]
        for k in range(kinds):
            m = [stored(fields + k, top + p * SUB, SUB) for p in range(len(parts))]
            for row in range(fields):
                part_sum = [None] * len(parts)
                for f in range(fields):
                    weight = mixer[(k * fields + row) * fields + f]
                    for p, part in enumerate(parts):
                        term = weight * turned[k, f, part]
                        part_sum[p] = term if f == 0 else part_sum[p] + term
                for p in range(len(parts)):
                    term = part_sum[p] * m[p]
                    acc[p][row] = term if k == 0 else acc[p][row] + term
        acc = [jnp.concatenate(list(rows_of), axis=0) for rows_of in zip(*acc)]
        fresh = []
        for f in range(fields):
            side = faces[0, f, GUARD + top - 1:GUARD + top - 1 + rows] + faces[1, f, GUARD + top + 1:GUARD + top + 1 + rows]
            new = u[f, at] + ((acc[f] + turned[kinds, f, at]) + side)
            if top < own or top + rows > own + count:
                new = new * stored(fields + kinds, top, rows)
            u[f, at] = new
            fresh.append(new)
        if first <= grp <= last:
            hi, lo = split((fresh[3] + fresh[4] + fresh[5]) * (1.0 / 3.0))
            xp[(grp - first) * TILE:(grp - first + 1) * TILE, 0:lanes] = hi
            xp[(grp - first) * TILE:(grp - first + 1) * TILE, lanes:] = lo
        for f in range(fields):
            new = fresh[f]
            if grp == 0:
                new = jnp.concatenate([zeros(margin, lanes), new], axis=0)
            if grp == groups - 1:
                new = jnp.concatenate([new, zeros(margin, lanes)], axis=0)
            put(grp, f, new)

    def sample(t):
        for c in range(COMPS):
            if c < 3:
                lhs = x[first:last + 1, c * TILE:(c + 1) * TILE].reshape(pick.shape[0], 2 * lanes)
            else:
                lhs = xp[...]
            prod = dot(lhs, ws[0:2 * lanes]) + dot(lhs[:, 0:lanes], ws[2 * lanes:])
            rows_out[t, c:c + 1, :] = jnp.sum(prod * pick[...], axis=0, keepdims=True)

    def step(todo, ahead, t, _):
        sample(t)
        for j, grp in enumerate(todo):
            spread(todo[(j + ahead) % len(todo)])
            advance(grp)
        return 0

    for grp in range(AHEAD):
        spread(grp)
    lax.fori_loop(0, WIDE, functools.partial(step, tuple(range(groups)), AHEAD), 0)
    between()
    lax.fori_loop(WIDE, STEPS, functools.partial(step, tuple(range(first, last + 1)), AHEAD - 1), 0)
    sample(STEPS)
    out[...] = zeros(*out.shape)
    for c in range(COMPS):
        for t in range(STEPS):
            out[c * STEPS + t:c * STEPS + t + 1, :] = rows_out[t + 1, c:c + 1, :]
    out[COMPS * STEPS:COMPS * STEPS + 1, :] = live[...]


def vm(x):
    return pltpu.with_memory_space_constraint(x, pltpu.VMEM)


def far(x):
    return pltpu.with_memory_space_constraint(x, pltpu.HBM)


VM = pl.BlockSpec(memory_space=pltpu.VMEM)


def shards(initial, derivative, coupling, face_lift, metric, rec_element, rec_weight, live_counts, shot_order, observed):
    fields, nodes, count = initial.shape
    lanes = -(-nodes // 128) * 128
    slots, width = observed.shape
    peers = lax.axis_size("mx")
    span = count + 2 * HALO
    kinds = derivative.shape[0]
    total = span + TILE
    picked = count + TILE
    wide = -(-(width + 1) // 64) * 64
    f32, bf16 = jnp.float32, jnp.bfloat16
    square = pltpu.VMEM((slots, slots), bf16)
    state, wb, ws, to_send, from_send, told, from_place, live, mixer, pick = pl.pallas_call(
        functools.partial(start_kernel, peers),
        out_shape=(
            pltpu.VMEM((fields + metric.shape[0] + 1, span, lanes), f32),
            pltpu.VMEM((3 * lanes, (kinds + 3) * lanes), bf16),
            pltpu.VMEM((3 * lanes, slots), bf16),
            square, square, pltpu.VMEM((peers, slots // peers // 2, lanes), f32), square,
            pltpu.VMEM((1, slots), f32),
            pltpu.VMEM((coupling.size, SUB, lanes), f32),
            pltpu.VMEM((picked, slots), f32),
        ),
        in_specs=[VM] * 10,
        out_specs=[VM] * 10,
        scratch_shapes=[
            pltpu.VMEM((lanes, lanes), f32),
            pltpu.VMEM((lanes, slots), f32),
            pltpu.SemaphoreType.DMA((2,)),
            pltpu.SemaphoreType.DMA((2,)),
        ],
        compiler_params=pltpu.CompilerParams(collective_id=0, has_side_effects=True, vmem_limit_bytes=GRANT),
        name="start",
    )(*(far(a) for a in (initial, metric, derivative, face_lift.transpose(1, 0, 2), rec_weight, shot_order.reshape(-1, lanes),
                    live_counts[None, :], rec_element[None, :], coupling.transpose(1, 0, 2), observed.T)))
    out, = pl.pallas_call(
        functools.partial(whole_kernel, peers),
        out_shape=(
            pltpu.VMEM((2 * width + 8, slots), f32),
        ),
        in_specs=[VM] * 11,
        out_specs=[VM],
        scratch_shapes=[
            pltpu.VMEM((fields, total, lanes), f32),
            pltpu.VMEM((total // TILE, fields * TILE, 2 * lanes), bf16),
            pltpu.VMEM((picked, 2 * lanes), bf16),
            pltpu.VMEM((kinds + 1, fields, total, lanes), f32),
            pltpu.VMEM((2, fields, total + 2 * GUARD, lanes), f32),
            pltpu.VMEM((STEPS + 1, 8, slots), f32),
            pltpu.VMEM((picked, slots), f32),
            pltpu.VMEM((coupling.size, SUB, lanes), f32),
            pltpu.VMEM((3 * lanes, (kinds + 3) * lanes), bf16),
            pltpu.VMEM((3 * lanes, slots), bf16),
            pltpu.VMEM((kinds + 1, span, lanes), f32),
            pltpu.VMEM((wide, slots), f32),
            pltpu.VMEM((2, peers, slots // peers // 2, lanes), f32),
            pltpu.VMEM((2, peers, slots // peers // 2, lanes), f32),
            pltpu.SemaphoreType.DMA((2, peers)),
            pltpu.SemaphoreType.DMA((2, peers)),
        ],
        compiler_params=pltpu.CompilerParams(collective_id=1, has_side_effects=True, vmem_limit_bytes=GRANT),
        name="whole",
    )(vm(state), vm(wb), vm(ws), vm(pick), vm(live), vm(mixer), far(observed.T), vm(to_send), vm(from_send), vm(told), vm(from_place))
    return out[:width].T, out[2 * width], out[width:2 * width].T


def solution(mesh):
    in_specs = (
        P("shots", None, "mx"),
        P(),
        P(),
        P(),
        P(None, "mx"),
        P("mx"),
        P(None, "mx"),
        P(),
        P(),
        P(("shots", "mx"), None),
    )
    out_specs = (P(("shots", "mx"), None), P(("shots", "mx")), P(("shots", "mx"), None))
    return jax.shard_map(shards, mesh=mesh, in_specs=in_specs, out_specs=out_specs, check_vma=False)
```

```python
import functools
import jax
import jax.numpy as jnp
from jax import lax
from jax.experimental import pallas as pl
from jax.experimental.pallas import tpu as pltpu
from jax.sharding import PartitionSpec as P

STEPS = 12
COMPS = 4
HALO = 16
REACH = 12
GUARD = 8
TILE = 16
SUB = 8
AHEAD = 3
WIDE = 4
GRANT = 32 * 2 ** 20


def split(x):
    hi = x.astype(jnp.bfloat16)
    return hi, (x - hi.astype(jnp.float32)).astype(jnp.bfloat16)


def zeros(*shape):
    return jnp.zeros(shape, jnp.float32)


def ones_where(cond):
    return jnp.where(cond, 1.0, 0.0).astype(jnp.bfloat16)


def dot(a, b):
    return jnp.dot(a, b, preferred_element_type=jnp.float32)


def permute(onehot, x):
    hi = x.astype(jnp.bfloat16)
    rest = x - hi.astype(jnp.float32)
    mid = rest.astype(jnp.bfloat16)
    low = (rest - mid.astype(jnp.float32)).astype(jnp.bfloat16)
    return dot(onehot, hi) + (dot(onehot, mid) + dot(onehot, low))


def greet(peers, me):
    barrier = pltpu.get_barrier_semaphore()

    def one(off, _):
        pl.semaphore_signal(barrier, inc=1, device_id={"mx": lax.rem(me + off, peers)}, device_id_type=pl.DeviceIdType.MESH)
        return 0

    lax.fori_loop(1, peers, one, 0)
    return barrier


def mirror(width):
    a = lax.broadcasted_iota(jnp.int32, (width, width), 0)
    b = lax.broadcasted_iota(jnp.int32, (width, width), 1)
    return ones_where((lax.div(a, STEPS) == lax.div(b, STEPS)) & (lax.rem(a, STEPS) + lax.rem(b, STEPS) == STEPS - 1))


def fold(rows, peers, lanes):
    slots, wide = rows.shape
    rows = jnp.concatenate([rows[:slots // 2], rows[slots // 2:]], axis=1)
    return rows.reshape(peers, slots // 2 // peers, lanes)


def start_kernel(peers, initial, metric, derivative, face_lift, weight_in, order, counts, elem, coupling, observed,
                 state, wb, ws, to_send, from_send, told, from_place, live, mixer, pick, kept,
                 pad, padw, send_sem, recv_sem):
    fields, nodes, count = initial.shape
    lanes = pad.shape[0]
    slots = padw.shape[1]
    pieces = slots // lanes
    pair = slots // peers
    me = lax.axis_index("mx")
    right, left = lax.rem(me + 1, peers), lax.rem(me + peers - 1, peers)
    barrier = pltpu.get_barrier_semaphore()
    sides = ((me < peers - 1, right), (me > 0, left))
    for there, side in sides:
        @pl.when(there)
        def hail():
            pl.semaphore_signal(barrier, inc=1, device_id={"mx": side}, device_id_type=pl.DeviceIdType.MESH)

    pad[...] = zeros(lanes, lanes)
    for f in range(fields):
        pad[0:nodes, :] = initial[f]
        state[f, HALO:HALO + count] = pad[...].T
    kinds = metric.shape[0]
    for k in range(kinds):
        state[fields + k, HALO:HALO + count] = jnp.broadcast_to(metric[k:k + 1, :], (lanes, count)).T
    pl.semaphore_wait(barrier, sum(there.astype(jnp.int32) for there, _ in sides))
    moved = fields + kinds
    copies = []
    for i, (side, at, to) in enumerate(((right, HALO + count - REACH, HALO - REACH), (left, HALO, HALO + count))):
        copies.append(pltpu.make_async_remote_copy(
            src_ref=state.at[0:moved, at:at + REACH], dst_ref=state.at[0:moved, to:to + REACH],
            send_sem=send_sem.at[i], recv_sem=recv_sem.at[i],
            device_id={"mx": side}, device_id_type=pl.DeviceIdType.MESH))

    state[0:moved, 0:HALO - REACH] = zeros(moved, HALO - REACH, lanes)
    state[0:moved, HALO + count + REACH:] = zeros(moved, HALO - REACH, lanes)
    for (there, _), copy, edge in zip(sides, copies, (HALO + count, HALO - REACH)):
        @pl.when(there)
        def send():
            copy.start()

        @pl.when(jnp.logical_not(there))
        def blank():
            state[0:moved, edge:edge + REACH] = zeros(moved, REACH, lanes)

    pad[...] = zeros(lanes, lanes)
    turns = derivative.shape[0]

    def weigh(k, matrix):
        pad[0:nodes, 0:nodes] = matrix
        hi, lo = split(pad[...].T * (0.5 / STEPS))
        at = slice(k * lanes, (k + 1) * lanes)
        wb[0:lanes, at] = hi
        wb[lanes:2 * lanes, at] = hi
        wb[2 * lanes:, at] = lo

    for k in range(turns):
        weigh(k, derivative[k])
    below, above = face_lift[:, 0, :], face_lift[:, 1, :]
    weigh(turns, below)
    weigh(turns + 1, above)
    weigh(turns + 2, -(below + above))
    padw[...] = zeros(lanes, slots)
    padw[0:nodes, :] = weight_in[...]
    hi, lo = split(padw[...])
    ws[0:lanes] = hi
    ws[lanes:2 * lanes] = hi
    ws[2 * lanes:] = lo
    rows = lax.broadcasted_iota(jnp.int32, (count + 2 * HALO, lanes), 0) + (me * count - HALO)
    state[moved] = jnp.where((rows >= 0) & (rows < count * peers), 1.0, 0.0)

    up = lax.broadcasted_iota(jnp.int32, (slots, slots), 0)
    across = lax.broadcasted_iota(jnp.int32, (slots, slots), 1)
    tri = ones_where(up <= across)
    blocks = jnp.concatenate([order[pl.ds(i, peers, stride=pieces), :] for i in range(pieces)], axis=1)
    source, slot = lax.div(blocks, slots), lax.rem(blocks, slots)
    mine = source == me
    rank = dot(ones_where(mine), tri) - 1.0
    rank = jnp.where(mine, rank, -1.0)
    tall = lax.broadcasted_iota(jnp.int32, (slots, peers), 0)
    wide = lax.broadcasted_iota(jnp.int32, (slots, peers), 1)
    half, upper = pair // 2, slots // 2
    repeat = ones_where(lax.div(lax.rem(tall, upper), half) == wide)
    rank_all = dot(repeat, rank.astype(jnp.bfloat16))
    slot_all = dot(repeat, slot.astype(jnp.float32).astype(jnp.bfloat16))
    hit = rank_all == (lax.div(up, upper) * half + lax.rem(up, half)).astype(jnp.float32)
    send_slot = jnp.sum(jnp.where(hit, slot_all, 0.0), axis=1, keepdims=True)
    sends = jnp.where(send_slot == across.astype(jnp.float32), 1.0, 0.0)
    to_send[...] = sends.astype(jnp.bfloat16)
    from_send[...] = sends.T.astype(jnp.bfloat16)
    own = jnp.concatenate([order[pl.ds(me * pieces + i, 1), :] for i in range(pieces)], axis=1)
    own_source = lax.div(own, slots)
    peer_ids = lax.broadcasted_iota(jnp.int32, (peers, slots), 0)
    from_peer = peer_ids == own_source
    seen = dot(ones_where(from_peer), tri) - 1.0
    own_rank = jnp.sum(jnp.where(from_peer, seen, 0.0), axis=0, keepdims=True)
    place = own_source.astype(jnp.float32) * float(half) + own_rank + jnp.where(own_rank >= float(half), float(upper - half), 0.0)
    places = jnp.where(up.astype(jnp.float32) == place, 1.0, 0.0)
    width = observed.shape[0]
    kept[...] = observed[...]
    mirrored = jnp.concatenate([permute(mirror(width), observed[...]), zeros(lanes // 2 - width, slots)], axis=0)
    told[...] = fold(permute(places.astype(jnp.bfloat16), mirrored.T), peers, lanes)
    from_place[...] = places.T.astype(jnp.bfloat16)
    here = lax.broadcasted_iota(jnp.int32, (1, peers), 1) == me
    limit = jnp.sum(jnp.where(here, counts[...].astype(jnp.float32), 0.0), axis=1, keepdims=True)
    alive = jnp.where(lax.broadcasted_iota(jnp.int32, (1, slots), 1).astype(jnp.float32) < limit, 1.0, 0.0)
    live[...] = alive
    ids = lax.broadcasted_iota(jnp.int32, pick.shape, 0) - (pick.shape[0] - count) // 2
    pick[...] = jnp.where(ids == elem[...], alive, 0.0)
    for row in range(fields):
        for k in range(kinds):
            line = coupling[row, k:k + 1, :]
            for f in range(fields):
                mixer[(k * fields + row) * fields + f] = jnp.broadcast_to(line[:, f:f + 1], (SUB, lanes))
    for (there, _), out, back in zip(sides, copies, copies[::-1]):
        @pl.when(there)
        def finish():
            out.wait_send()
            back.wait_recv()


def unfold(block, wide):
    rows = block.reshape(block.shape[0] * block.shape[1], block.shape[2])
    return jnp.concatenate([rows[:, 0:wide], rows[:, wide:]], axis=0)


def whole_kernel(peers, state, wb_in, ws_in, pick_in, live, mixer_in, observed, to_send, from_send, told, from_place,
                 outs, u, x, xp, turned, faces, rows_out, pick, mixer, wb, ws, held, traces,
                 sent, got, send_sem, recv_sem):
    width, slots = observed.shape
    residual, misfit, adjoint = outs.at[0:width], outs.at[2 * width:2 * width + 1], outs.at[width:2 * width]
    lanes = sent.shape[-1]
    wide = traces.shape[0]
    me = lax.axis_index("mx")
    barrier = greet(peers, me)
    sent[0] = told[...]
    back = mirror(width)

    def offset(i):
        return 1 + lax.rem(i + peers // 2 - 1, peers - 1)

    def copy_to(which, i):
        dest = lax.rem(me + offset(i), peers)
        return pltpu.make_async_remote_copy(
            src_ref=sent.at[which, dest], dst_ref=got.at[which, me],
            send_sem=send_sem.at[which, dest], recv_sem=recv_sem.at[which, me],
            device_id={"mx": dest}, device_id_type=pl.DeviceIdType.MESH)

    def copy_from(which, i):
        src = lax.rem(me - offset(i) + peers, peers)
        return pltpu.make_async_remote_copy(
            src_ref=sent.at[which, src], dst_ref=got.at[which, src],
            send_sem=send_sem.at[which, src], recv_sem=recv_sem.at[which, src],
            device_id={"mx": src}, device_id_type=pl.DeviceIdType.MESH)

    def begin(which, i, _):
        copy_to(which, i).start()
        return 0

    def finish(which, i, _):
        copy_from(which, i).wait_recv()
        return 0

    def drain(which, i, _):
        copy_to(which, i).wait_send()
        return 0

    def each(action, which):
        lax.fori_loop(0, peers - 1, functools.partial(action, which), 0)

    def between():
        pl.semaphore_wait(barrier, peers - 1)
        each(begin, 0)
        got[0, pl.ds(me, 1)] = sent[0, pl.ds(me, 1)]

    wave_part(between, state, wb_in, ws_in, pick_in, live, mixer_in, traces, u, x, xp, turned, faces, rows_out, pick, mixer, wb, ws, held)
    sent[1] = fold(permute(to_send[...], traces[...].T), peers, lanes)
    each(begin, 1)
    got[1, pl.ds(me, 1)] = sent[1, pl.ds(me, 1)]
    each(finish, 0)
    slot_obs = permute(from_send[...], unfold(got[0], wide)).T
    mine = traces[width:width + 1, :]
    adjoint[...] = mine * (permute(back, traces[0:width, :]) - slot_obs[0:width])
    each(drain, 0)
    each(finish, 1)
    placed = permute(from_place[...], unfold(got[1], wide)).T
    res = placed[width:width + 1] * (placed[:width] - observed[...])
    residual[...] = res
    misfit[...] = 0.5 * jnp.sum(res * res, axis=0, keepdims=True)
    each(drain, 1)


def wave_part(between, state, wb_in, ws_in, pick_in, live, mixer_in, out, u, x, xp, turned, faces, rows_out, pick, mixer, wb, ws, held):
    fields, total, lanes = u.shape
    span = state.shape[1]
    count = span - 2 * HALO
    kinds = turned.shape[0] - 1
    margin = (total - span) // 2
    own = margin + HALO
    slots = ws.shape[1]
    groups = total // TILE

    def stored(f, r, n):
        return held[f - fields, r - margin:r - margin + n]

    wb[...] = wb_in[...]
    ws[...] = ws_in[...]
    held[...] = state[fields:]

    def put(grp, f, new):
        hi, lo = split(new)
        x[grp, f * TILE:(f + 1) * TILE, 0:lanes] = hi
        x[grp, f * TILE:(f + 1) * TILE, lanes:] = lo

    for f in range(fields):
        u[f, 0:margin] = zeros(margin, lanes)
        u[f, total - margin:] = zeros(margin, lanes)
        u[f, margin:total - margin] = state[f] * state[fields + kinds]
        for k in range(2):
            faces[k, f, 0:GUARD] = zeros(GUARD, lanes)
            faces[k, f, GUARD + total:] = zeros(GUARD, lanes)
        for grp in range(groups):
            put(grp, f, u[f, grp * TILE:(grp + 1) * TILE])

    first, last = own // TILE, (own + count - 1) // TILE
    xp[...] = jnp.zeros(xp.shape, xp.dtype)
    pick[...] = pick_in[...]
    mixer[...] = mixer_in[...]

    def spread(grp):
        lhs = x[grp]
        res = dot(lhs, wb[0:2 * lanes]) + dot(lhs[:, 0:lanes], wb[2 * lanes:])
        at = slice(grp * TILE, (grp + 1) * TILE)
        shifted = slice(GUARD + grp * TILE, GUARD + (grp + 1) * TILE)
        for f in range(fields):
            part = res[f * TILE:(f + 1) * TILE]
            for k in range(kinds):
                turned[k, f, at] = part[:, k * lanes:(k + 1) * lanes]
            for k in range(2):
                faces[k, f, shifted] = part[:, (kinds + k) * lanes:(kinds + k + 1) * lanes]
            turned[kinds, f, at] = part[:, (kinds + 2) * lanes:]

    def advance(grp):
        top, rows = grp * TILE, TILE
        if grp == 0:
            top, rows = top + margin, rows - margin
        if grp == groups - 1:
            rows = rows - margin
        at = slice(top, top + rows)
        parts = [slice(top + r, top + r + SUB) for r in range(0, rows, SUB)]
        acc = [[None] * fields for _ in parts]
        for k in range(kinds):
            m = [stored(fields + k, top + p * SUB, SUB) for p in range(len(parts))]
            for row in range(fields):
                part_sum = [None] * len(parts)
                for f in range(fields):
                    weight = mixer[(k * fields + row) * fields + f]
                    for p, part in enumerate(parts):
                        term = weight * turned[k, f, part]
                        part_sum[p] = term if f == 0 else part_sum[p] + term
                for p in range(len(parts)):
                    term = part_sum[p] * m[p]
                    acc[p][row] = term if k == 0 else acc[p][row] + term
        acc = [jnp.concatenate(list(rows_of), axis=0) for rows_of in zip(*acc)]
        fresh = []
        for f in range(fields):
            side = faces[0, f, GUARD + top - 1:GUARD + top - 1 + rows] + faces[1, f, GUARD + top + 1:GUARD + top + 1 + rows]
            new = u[f, at] + ((acc[f] + turned[kinds, f, at]) + side)
            if top < own or top + rows > own + count:
                new = new * stored(fields + kinds, top, rows)
            u[f, at] = new
            fresh.append(new)
        if first <= grp <= last:
            hi, lo = split((fresh[3] + fresh[4] + fresh[5]) * (1.0 / 3.0))
            xp[(grp - first) * TILE:(grp - first + 1) * TILE, 0:lanes] = hi
            xp[(grp - first) * TILE:(grp - first + 1) * TILE, lanes:] = lo
        for f in range(fields):
            new = fresh[f]
            if grp == 0:
                new = jnp.concatenate([zeros(margin, lanes), new], axis=0)
            if grp == groups - 1:
                new = jnp.concatenate([new, zeros(margin, lanes)], axis=0)
            put(grp, f, new)

    def sample(t):
        for c in range(COMPS):
            if c < 3:
                lhs = x[first:last + 1, c * TILE:(c + 1) * TILE].reshape(pick.shape[0], 2 * lanes)
            else:
                lhs = xp[...]
            prod = dot(lhs, ws[0:2 * lanes]) + dot(lhs[:, 0:lanes], ws[2 * lanes:])
            rows_out[t, c:c + 1, :] = jnp.sum(prod * pick[...], axis=0, keepdims=True)

    def step(todo, ahead, t, _):
        sample(t)
        for j, grp in enumerate(todo):
            spread(todo[(j + ahead) % len(todo)])
            advance(grp)
        return 0

    for grp in range(AHEAD):
        spread(grp)
    lax.fori_loop(0, WIDE, functools.partial(step, tuple(range(groups)), AHEAD), 0)
    between()
    lax.fori_loop(WIDE, STEPS, functools.partial(step, tuple(range(first, last + 1)), AHEAD - 1), 0)
    sample(STEPS)
    out[...] = zeros(*out.shape)
    for c in range(COMPS):
        for t in range(STEPS):
            out[c * STEPS + t:c * STEPS + t + 1, :] = rows_out[t + 1, c:c + 1, :]
    out[COMPS * STEPS:COMPS * STEPS + 1, :] = live[...]


def vm(x):
    return pltpu.with_memory_space_constraint(x, pltpu.VMEM)


def far(x):
    return pltpu.with_memory_space_constraint(x, pltpu.HBM)


VM = pl.BlockSpec(memory_space=pltpu.VMEM)


def shards(initial, derivative, coupling, face_lift, metric, rec_element, rec_weight, live_counts, shot_order, observed):
    fields, nodes, count = initial.shape
    lanes = -(-nodes // 128) * 128
    slots, width = observed.shape
    peers = lax.axis_size("mx")
    span = count + 2 * HALO
    kinds = derivative.shape[0]
    total = span + TILE
    picked = count + TILE
    wide = -(-(width + 1) // 64) * 64
    f32, bf16 = jnp.float32, jnp.bfloat16
    square = pltpu.VMEM((slots, slots), bf16)
    state, wb, ws, to_send, from_send, told, from_place, live, mixer, pick, kept = pl.pallas_call(
        functools.partial(start_kernel, peers),
        out_shape=(
            pltpu.VMEM((fields + metric.shape[0] + 1, span, lanes), f32),
            pltpu.VMEM((3 * lanes, (kinds + 3) * lanes), bf16),
            pltpu.VMEM((3 * lanes, slots), bf16),
            square, square, pltpu.VMEM((peers, slots // peers // 2, lanes), f32), square,
            pltpu.VMEM((1, slots), f32),
            pltpu.VMEM((coupling.size, SUB, lanes), f32),
            pltpu.VMEM((picked, slots), f32),
            pltpu.VMEM((width, slots), f32),
        ),
        in_specs=[VM] * 10,
        out_specs=[VM] * 11,
        scratch_shapes=[
            pltpu.VMEM((lanes, lanes), f32),
            pltpu.VMEM((lanes, slots), f32),
            pltpu.SemaphoreType.DMA((2,)),
            pltpu.SemaphoreType.DMA((2,)),
        ],
        compiler_params=pltpu.CompilerParams(collective_id=0, has_side_effects=True, vmem_limit_bytes=GRANT),
        name="start",
    )(*(far(a) for a in (initial, metric, derivative, face_lift.transpose(1, 0, 2), rec_weight, shot_order.reshape(-1, lanes),
                    live_counts[None, :], rec_element[None, :], coupling.transpose(1, 0, 2), observed.T)))
    out, = pl.pallas_call(
        functools.partial(whole_kernel, peers),
        out_shape=(
            pltpu.VMEM((2 * width + 8, slots), f32),
        ),
        in_specs=[VM] * 11,
        out_specs=[VM],
        scratch_shapes=[
            pltpu.VMEM((fields, total, lanes), f32),
            pltpu.VMEM((total // TILE, fields * TILE, 2 * lanes), bf16),
            pltpu.VMEM((picked, 2 * lanes), bf16),
            pltpu.VMEM((kinds + 1, fields, total, lanes), f32),
            pltpu.VMEM((2, fields, total + 2 * GUARD, lanes), f32),
            pltpu.VMEM((STEPS + 1, 8, slots), f32),
            pltpu.VMEM((picked, slots), f32),
            pltpu.VMEM((coupling.size, SUB, lanes), f32),
            pltpu.VMEM((3 * lanes, (kinds + 3) * lanes), bf16),
            pltpu.VMEM((3 * lanes, slots), bf16),
            pltpu.VMEM((kinds + 1, span, lanes), f32),
            pltpu.VMEM((wide, slots), f32),
            pltpu.VMEM((2, peers, slots // peers // 2, lanes), f32),
            pltpu.VMEM((2, peers, slots // peers // 2, lanes), f32),
            pltpu.SemaphoreType.DMA((2, peers)),
            pltpu.SemaphoreType.DMA((2, peers)),
        ],
        compiler_params=pltpu.CompilerParams(collective_id=1, has_side_effects=True, vmem_limit_bytes=GRANT),
        name="whole",
    )(vm(state), vm(wb), vm(ws), vm(pick), vm(live), vm(mixer), vm(kept), vm(to_send), vm(from_send), vm(told), vm(from_place))
    return out[:width].T, out[2 * width], out[width:2 * width].T


def solution(mesh):
    in_specs = (
        P("shots", None, "mx"),
        P(),
        P(),
        P(),
        P(None, "mx"),
        P("mx"),
        P(None, "mx"),
        P(),
        P(),
        P(("shots", "mx"), None),
    )
    out_specs = (P(("shots", "mx"), None), P(("shots", "mx")), P(("shots", "mx"), None))
    return jax.shard_map(shards, mesh=mesh, in_specs=in_specs, out_specs=out_specs, check_vma=False)
```
